512 devices in a mesh: dom: 64 (over z_lo, y, core), ch: 8 (over z_hi, x).
Axes of the slice: x: 4, y: 8, z: 8 (z_hi: 2, z_lo: 4; z = z_hi * 4 + z_lo), core: 2. Of those that a mesh axis runs over, the one named last changes fastest.
Arguments:
- node_irreps: bfloat16 [49, 128, 1024], P(None, 'ch', 'dom'), may hold values from -6 to 6
- out_grad: bfloat16 [49, 128, 1024], P(None, 'ch', 'dom'), may hold values from -6 to 6
- edge_source: int32 [8, 1024], P(None, 'dom'), may hold values from 0 to 31
- edge_rotation: int32 [8, 1024], P(None, 'dom'), may hold values from 0 to 255
- edge_count: int32 [1024], P('dom'), may hold values from 1 to 8
- ghost_slot: int32 [1024], P('dom'), may hold values from 0 to 15, as said below
- wigner: float32 [455, 16384], P(None, 'dom'), may hold values from -1 to 1, as said below
- so2_m0: bfloat16 [7, 128, 7, 128], P(None, 'ch'), may hold values from -0.1875 to 0.1875
- so2_m1: bfloat16 [2, 6, 128, 6, 128], P(None, None, 'ch'), may hold values from -0.15625 to 0.15625
- so2_m2: bfloat16 [2, 5, 128, 5, 128], P(None, None, 'ch'), may hold values from -0.15625 to 0.15625
- attn_vector: float32 [128], P('ch'), may hold values from -60 to 60
Outputs:
- updated: bfloat16 [49, 128, 1024], P(None, 'ch', 'dom')
- irreps_grad: float32 [49, 128, 1024], P(None, 'ch', 'dom')
The draws below stay inside these ranges and needn't reach their ends.
Inputs may be any that keep to these rules, and one draw needn't show every extreme that they name: `edge_source`: slots below 16 are the domain's own atoms in order; slot 16 + g is the domain's ghost g. `edge_rotation`: picks one of the 256 columns of wigner that belong to the atom's domain. Slots j < edge_count[a] are live, the others padding. `ghost_slot`: of a domain's 16 entries, the first 8 name atoms of the previous domain (cyclically) among its last 16 slots, the others atoms of the next domain among its first 16 slots. `wigner`: each column holds for l = 0..6 an orthogonal (2l+1) x (2l+1) block, row-major, blocks in order of l.
All inputs are finite; a program needn't handle non-finite values.
Results may differ from the reference program's by a relative error of at most 0.012.
The reference program's roundings to bfloat16 on the way (of `rot`) count: a program that leaves them out, or rounds other values in their place, can miss the bound.
Values may be sent and summed in bfloat16 or wider, within the bound.
A program may use at most 128 MiB of HBM per device.

```python
import jax
import jax.numpy as jnp
from jax import lax

C = 128
HEADS = 8
LMAX = 6
MMAX = 2
OWN = 16
NB = 8
GH = 16
RIM = 16
ROT_DOM = 256
K = 49
HEAD_CH = 16
ATOMS = 1024
ROTATIONS = 16384
N_DOM = 64
N_CH = 8


def draw_ghost_slot(key, part):
    half = GH // 2
    low = jax.random.randint(jax.random.fold_in(key, 101), (N_DOM, half), OWN - RIM, OWN, dtype=jnp.int32)
    high = jax.random.randint(jax.random.fold_in(key, 102), (N_DOM, GH - half), 0, RIM, dtype=jnp.int32)
    return jnp.concatenate([low, high], 1).reshape(N_DOM * GH)


def draw_wigner(key, part):
    pieces = []
    for level in range(LMAX + 1):
        width = 2 * level + 1
        raw = jax.random.normal(jax.random.fold_in(key, 211 + level), (ROTATIONS, width, width), jnp.float32) * 0.6
        skewed = raw - jnp.swapaxes(raw, 1, 2)
        eye = jnp.broadcast_to(jnp.eye(width, dtype=jnp.float32), (ROTATIONS, width, width))
        ortho = jnp.linalg.solve(eye + skewed, eye - skewed)
        pieces.append(ortho.reshape(ROTATIONS, width * width).T)
    return jnp.concatenate(pieces, 0).astype(jnp.float32)


def draw_attn_vector(key, part):
    base = jnp.clip(jax.random.normal(jax.random.fold_in(key, 301), (C,), jnp.float32), -4.0, 4.0) * HEAD_CH ** (-0.5)
    return base.astype(jnp.float32)


def touch_ends(result, key, low, high):
    spot = [jax.random.randint(jax.random.fold_in(key, axis), (), 0, length) for axis, length in enumerate(result.shape)]
    longest = result.shape.index(max(result.shape))
    beside = spot[:longest] + [(spot[longest] + 1) % result.shape[longest]] + spot[longest + 1:]
    return result.at[tuple(spot)].set(low).at[tuple(beside)].set(high)


def level_of(key, dims, cuts, least, top_value):
    gain = 1.0
    for dim, blocks in cuts:
        heights = jax.random.uniform(jax.random.fold_in(jax.random.fold_in(key, 6), dim), (blocks,), jnp.float32, least / len(cuts), top_value / len(cuts))
        gain = gain * jnp.repeat(jnp.exp(heights), dims[dim] // blocks).reshape((-1,) + (1,) * (len(dims) - 1 - dim))
    return gain


def noise(key, shape, scale, most, split=(), kind=jnp.bfloat16):
    drawn = jax.random.normal(key, shape, jnp.float32) * scale
    if len(split) > 0:
        drawn = level_of(key, shape, split, -0.22, 0.18) * drawn
    return jnp.clip(drawn, min=-most, max=most).astype(kind)


def setup_inputs(seed: int = 0) -> dict:
    key_of = jax.random.split(jax.random.key(seed), 12)
    return {
        "node_irreps": noise(key_of[0], (K, C, ATOMS), 1.0, 6.0, ((1, 8), (2, 64))),
        "out_grad": noise(key_of[1], (K, C, ATOMS), 1.0, 6.0, ((1, 8), (2, 64))),
        "edge_source": touch_ends(jax.random.randint(key_of[2], (NB, ATOMS), 0, OWN + GH), jax.random.fold_in(key_of[2], 1), 0, (OWN + GH) - 1).astype(jnp.int32),
        "edge_rotation": touch_ends(jax.random.randint(key_of[3], (NB, ATOMS), 0, ROT_DOM), jax.random.fold_in(key_of[3], 1), 0, ROT_DOM - 1).astype(jnp.int32),
        "edge_count": touch_ends(jax.random.randint(key_of[4], (ATOMS,), 1, NB + 1), jax.random.fold_in(key_of[4], 1), 1, NB).astype(jnp.int32),
        "ghost_slot": draw_ghost_slot(jax.random.fold_in(key_of[11], 71), 0),
        "wigner": draw_wigner(jax.random.fold_in(key_of[11], 71), 0),
        "so2_m0": noise(key_of[7], (LMAX + 1, C, LMAX + 1, C), ((LMAX + 1) * C) ** -0.5, 0.1875, ((1, 8),)),
        "so2_m1": noise(key_of[8], (2, LMAX, C, LMAX, C), (2 * LMAX * C) ** -0.5, 0.15625, ((2, 8),)),
        "so2_m2": noise(key_of[9], (2, LMAX - 1, C, LMAX - 1, C), (2 * (LMAX - 1) * C) ** -0.5, 0.15625, ((2, 8),)),
        "attn_vector": draw_attn_vector(jax.random.fold_in(key_of[11], 71), 0),
    }


def plan_tables(degree_top, order_top):
    blocks = []
    offset = 0
    lmajor = []
    for level in range(degree_top + 1):
        width = 2 * level + 1
        reach = min(level, order_top)
        kept = [level + order for order in range(-reach, reach + 1)]
        blocks.append((level, width, offset, kept))
        for order in range(-reach, reach + 1):
            lmajor.append((level, order))
        offset += width * width
    grouped = [(level, 0) for level in range(degree_top + 1)]
    for order in range(1, order_top + 1):
        grouped += [(level, order) for level in range(order, degree_top + 1)]
        grouped += [(level, -order) for level in range(order, degree_top + 1)]
    to_group = [lmajor.index(entry) for entry in grouped]
    to_major = [grouped.index(entry) for entry in lmajor]
    return (blocks, to_group, to_major)

def rotate_in(feats, wig_edges, blocks, to_group):
    parts = []
    for level, width, offset, kept in blocks:
        for row in kept:
            acc = wig_edges[offset + row * width][None, :] * feats[level * level]
            for col in range(1, width):
                acc = acc + wig_edges[offset + row * width + col][None, :] * feats[level * level + col]
            parts.append(acc)
    return jnp.stack([parts[i] for i in to_group])

def rotate_out(values, wig_edges, blocks, to_major):
    rows = [values[i] for i in to_major]
    out = []
    pos = 0
    for level, width, offset, kept in blocks:
        mine = rows[pos:pos + len(kept)]
        pos += len(kept)
        for col in range(width):
            acc = wig_edges[offset + kept[0] * width + col][None, :] * mine[0]
            for j in range(1, len(kept)):
                acc = acc + wig_edges[offset + kept[j] * width + col][None, :] * mine[j]
            out.append(acc)
    return jnp.stack(out)

def so2_mix(rot, w_zero, w_one, w_two, degree_top):
    chans = rot.shape[1]
    edges = rot.shape[2]
    group = w_zero.shape[1]
    first = degree_top + 1
    outs = [jnp.dot(w_zero.reshape(first * group, first * chans).astype(jnp.float32), rot[:first].reshape(first * chans, edges).astype(jnp.float32), preferred_element_type=jnp.float32).reshape(first, group, edges)]
    pos = first
    for order, weights in ((1, w_one), (2, w_two)):
        count = degree_top + 1 - order
        plus = rot[pos:pos + count].reshape(count * chans, edges)
        minus = rot[pos + count:pos + 2 * count].reshape(count * chans, edges)
        real = weights[0].reshape(count * group, count * chans)
        imag = weights[1].reshape(count * group, count * chans)
        y_plus = jnp.dot(real.astype(jnp.float32), plus.astype(jnp.float32), preferred_element_type=jnp.float32) - jnp.dot(imag.astype(jnp.float32), minus.astype(jnp.float32), preferred_element_type=jnp.float32)
        y_minus = jnp.dot(real.astype(jnp.float32), minus.astype(jnp.float32), preferred_element_type=jnp.float32) + jnp.dot(imag.astype(jnp.float32), plus.astype(jnp.float32), preferred_element_type=jnp.float32)
        outs += [y_plus.reshape(count, group, edges), y_minus.reshape(count, group, edges)]
        pos += 2 * count
    return jnp.concatenate(outs, 0)

def attend_tail(rot32, wig_edges, counts, w_zero, w_one, w_two, attn, heads_here, blocks, to_major, degree_top):
    rot = rot32.astype(jnp.bfloat16)
    mixed = so2_mix(rot, w_zero, w_one, w_two, degree_top)
    scalar = mixed[0]
    values = mixed * jax.nn.sigmoid(scalar)[None]
    group, edges = scalar.shape
    atoms_here = counts.shape[0]
    slots = edges // atoms_here
    score = (jax.nn.silu(scalar) * attn[:, None]).reshape(heads_here, group // heads_here, edges).sum(1)
    score = score.reshape(heads_here, slots, atoms_here)
    live = (lax.broadcasted_iota(jnp.int32, (slots, atoms_here), 0) < counts[None, :])[None]
    top = lax.optimization_barrier(jnp.max(jnp.where(live, score, -1e+30), axis=1, keepdims=True))
    weight = jnp.exp(jnp.where(live, score - top, -1e+30))
    weight = weight / lax.optimization_barrier(jnp.sum(weight, axis=1, keepdims=True))
    spread = jnp.broadcast_to(weight.reshape(heads_here, 1, edges), (heads_here, group // heads_here, edges)).reshape(group, edges)
    back = rotate_out(values * spread[None], wig_edges, blocks, to_major)
    return back.reshape(back.shape[0], group, slots, atoms_here).sum(2)

def reference(node_irreps, out_grad, edge_source, edge_rotation, edge_count, ghost_slot, wigner, so2_m0, so2_m1, so2_m2, attn_vector):
    blocks, to_group, to_major = plan_tables(LMAX, MMAX)
    group = C // N_CH
    heads_here = HEADS // N_CH
    slots = ghost_slot.reshape(N_DOM, GH)
    half = GH // 2

    def one_domain(x32, d):
        lower = jnp.mod(d - 1, N_DOM).astype(jnp.int32)
        upper = jnp.mod(d + 1, N_DOM).astype(jnp.int32)
        own = lax.dynamic_slice_in_dim(x32, (d * OWN).astype(jnp.int32), OWN, 2)
        below = jnp.take(lax.dynamic_slice_in_dim(x32, (lower * OWN).astype(jnp.int32), OWN, 2), slots[d, :half], axis=2)
        above = jnp.take(lax.dynamic_slice_in_dim(x32, (upper * OWN).astype(jnp.int32), OWN, 2), slots[d, half:], axis=2)
        table = jnp.concatenate([own, below, above], 2)
        source = lax.dynamic_slice_in_dim(edge_source, (d * OWN).astype(jnp.int32), OWN, 1).reshape(-1)
        turn = lax.dynamic_slice_in_dim(edge_rotation, (d * OWN).astype(jnp.int32), OWN, 1).reshape(-1)
        counts = lax.dynamic_slice_in_dim(edge_count, (d * OWN).astype(jnp.int32), OWN, 0)
        table_rot = lax.dynamic_slice_in_dim(wigner, (d * ROT_DOM).astype(jnp.int32), ROT_DOM, 1)
        wig_edges = jnp.take(table_rot, turn, axis=1)
        feats = jnp.take(table, source, axis=2)
        outs = []
        for index in range(N_CH):
            lo = index * group
            rot32 = rotate_in(feats, wig_edges, blocks, to_group)
            outs.append(attend_tail(rot32, wig_edges, counts, so2_m0[:, lo:lo + group], so2_m1[:, :, lo:lo + group], so2_m2[:, :, lo:lo + group], attn_vector[lo:lo + group], heads_here, blocks, to_major, LMAX))
        return jnp.concatenate(outs, 1)

    def forward(x32):
        stacked = lax.map(lambda d: jax.checkpoint(one_domain)(x32, d), jnp.arange(N_DOM, dtype=jnp.int32))
        return jnp.transpose(stacked, (1, 2, 0, 3)).reshape(K, C, ATOMS)
    x32 = node_irreps.astype(jnp.float32)
    agg, pullback = jax.vjp(forward, x32)
    updated = (x32 + agg).astype(jnp.bfloat16)
    grad32 = out_grad.astype(jnp.float32)
    irreps_grad = grad32 + pullback(grad32)[0]
    return (updated, irreps_grad)
```

```python
import jax
import jax.numpy as jnp
from jax import lax
from jax.experimental import pallas as pl
from jax.experimental.pallas import tpu as pltpu
from jax.sharding import PartitionSpec as P

LMAX = 6
MMAX = 2
K = 49
OWN = 16
EDGES = 128
KP = 56
ROWS = 2 * KP
PITCH = 116
F32 = jnp.float32
BF16 = jnp.bfloat16
MESH = pl.DeviceIdType.MESH


def rows_of_levels():
    levels = []
    offset = 0
    for level in range(LMAX + 1):
        width = 2 * level + 1
        reach = min(level, MMAX)
        orders = list(range(-reach, reach + 1))
        levels.append((level, width, offset, orders))
        offset += width * width
    return levels


LEVELS = rows_of_levels()


def place(level, order):
    if order == 0:
        return level
    if order == 1:
        return 6 + level
    if order == -1:
        return 12 + level
    if order == 2:
        return 17 + level
    return 22 + level


def iota(shape, dim):
    return lax.broadcasted_iota(jnp.int32, shape, dim)


def one_where(cond):
    return jnp.where(cond, 1.0, 0.0).astype(BF16)


def spin(x, shift):
    return pltpu.roll(x, shift, 1)


def dot(a, b):
    return jnp.dot(a, b, preferred_element_type=F32)


def turn(wige, level, width, offset, order, col):
    row = offset + (level + order) * width + col
    return jnp.broadcast_to(wige[row : row + 1, :], (8, EDGES))


def rotate_in(mixed, wige, feats, write):
    for c in range(8):
        feats[c * PITCH : c * PITCH + ROWS, :] = mixed[:, c * EDGES : (c + 1) * EDGES]
    for level, width, offset, orders in LEVELS:
        acc = {}
        for col in range(width):
            k = level * level + col
            low = feats[pl.ds(k, 8, stride=PITCH), :]
            high = feats[pl.ds(KP + k, 8, stride=PITCH), :]
            for order in orders:
                w = turn(wige, level, width, offset, order, col)
                if col == 0:
                    acc[order] = (w * low, w * high)
                else:
                    a, b = acc[order]
                    acc[order] = (a + w * low, b + w * high)
        for order in orders:
            write(place(level, order), jnp.concatenate(acc[order], 0))


def rotate_out(read, wige, back):
    for level, width, offset, orders in LEVELS:
        mine = {order: read(place(level, order)) for order in orders}
        for col in range(width):
            k = level * level + col
            low = high = None
            for order in orders:
                w = turn(wige, level, width, offset, order, col)
                a, b = mine[order]
                low = w * a if low is None else low + w * a
                high = w * b if high is None else high + w * b
            back[pl.ds(k, 8, stride=PITCH), :] = low
            back[pl.ds(KP + k, 8, stride=PITCH), :] = high


def across(back):
    return jnp.concatenate([back[c * PITCH : c * PITCH + ROWS, :] for c in range(8)], 1)


def to_rows(ref, pad):
    pad[...] = jnp.zeros_like(pad)
    pad[:, 0:K] = ref[...].astype(F32).reshape(256, K)
    low = pad[0:128, :].T
    high = pad[128:256, :].T
    return jnp.concatenate([low[0:KP], high[0:KP]], 0)


def from_rows(rows):
    fill = jnp.zeros((128 - KP, 128), F32)
    low = jnp.concatenate([rows[0:KP], fill], 0).T
    high = jnp.concatenate([rows[KP:ROWS], fill], 0).T
    return jnp.concatenate([low, high], 0)[:, 0:K].reshape(16, 16, K)


def body(
    x_ref,
    g_ref,
    src_ref,
    turn_ref,
    cnt_ref,
    slot_ref,
    wig_ref,
    w0_ref,
    w1_ref,
    w2_ref,
    attn_ref,
    upd_ref,
    grad_ref,
    tab,
    pad,
    wige,
    gat,
    sca,
    gat_tile,
    sca_tile,
    feats,
    back,
    rot,
    drot,
    ys,
    ps,
    wt0,
    wt1,
    wt2,
    accum,
    below_out,
    above_out,
    from_above,
    from_below,
    x_out,
    x_in,
    z_out,
    z_in,
    red,
    send_sem,
    tab_sem,
    ghost_send,
    ghost_recv,
    xs_send,
    xs_recv,
    zs_send,
    zs_recv,
):
    doms = lax.axis_size("dom")
    d = lax.axis_index("dom")
    ch = lax.axis_index("ch")
    zh = ch // 4
    xi = lax.rem(ch, 4)
    up = (lax.rem(d + 1, doms), ch)
    down = (lax.rem(d + doms - 1, doms), ch)
    other = (d, lax.rem(ch + 4, 8))

    def peer(off):
        return (d, zh * 4 + lax.rem(xi + off, 4))

    barrier = pltpu.get_barrier_semaphore()
    for target in (up, down, other, peer(1), peer(2), peer(3)):
        pl.semaphore_signal(barrier, inc=1, device_id=target, device_id_type=MESH)

    tab[0, ch] = to_rows(x_ref, pad).astype(BF16)

    def rcopy(src, dst, ssem, rsem, target):
        return pltpu.make_async_remote_copy(
            src_ref=src,
            dst_ref=dst,
            send_sem=ssem,
            recv_sem=rsem,
            device_id=target,
            device_id_type=MESH,
        )

    def table_copy(blk, who, n, target):
        return rcopy(
            tab.at[0, who], tab.at[blk, who], send_sem.at[n], tab_sem.at[blk, who], target
        )

    def arrival(blk, who):
        return rcopy(
            tab.at[0, who], tab.at[blk, who], send_sem.at[0], tab_sem.at[blk, who], up
        ).wait_recv()

    pl.semaphore_wait(barrier, 6)
    sends = []

    def go(blk, who, target):
        copy = table_copy(blk, who, len(sends), target)
        copy.start()
        sends.append(copy)

    go(0, ch, other)
    for off in (2, 1, 3):
        go(0, ch, peer(off))
    go(1, ch, up)
    go(2, ch, down)

    spread = one_where(lax.rem(iota((16, EDGES), 1), 16) == iota((16, EDGES), 0))
    pick = (iota((8, EDGES), 1) // 16) == iota((8, EDGES), 0)

    def edge_row(ref):
        wide = dot(ref[...].astype(F32).astype(BF16), spread)
        return jnp.sum(jnp.where(pick, wide, 0.0), axis=0, keepdims=True)

    src = edge_row(src_ref)
    turns = edge_row(turn_ref)
    lane = iota((1, EDGES), 1)
    atom = lax.rem(lane, 16)
    ghost = jnp.zeros((1, EDGES), F32)
    count = jnp.zeros((1, EDGES), jnp.int32)
    for a in range(16):
        ghost = jnp.where(src == 16.0 + a, slot_ref[a].astype(F32), ghost)
        count = jnp.where(atom == a, cnt_ref[a], count)
    nowhere = -1000.0
    index = (
        jnp.where(src < 16.0, src, nowhere),
        jnp.where((src >= 16.0) & (src < 24.0), ghost, nowhere),
        jnp.where(src >= 24.0, ghost, nowhere),
    )
    row_id = iota((EDGES, EDGES), 0).astype(F32)
    lane_id = iota((EDGES, EDGES), 1).astype(F32)
    for blk in range(4):
        idx = atom.astype(F32) if blk == 3 else index[blk]
        wide = jnp.broadcast_to(idx, (EDGES, EDGES))
        tall = wide.T
        for c in range(8):
            forth = one_where(row_id == wide + 16.0 * c)
            fro = one_where(lane_id == tall + 16.0 * c)
            if blk == 3:
                gat_tile[:, c * 128 : c * 128 + 128] = forth
                sca_tile[c * 128 : c * 128 + 128, :] = fro
            else:
                gat[blk * 128 : blk * 128 + 128, c * 128 : c * 128 + 128] = forth
                sca[c * 128 : c * 128 + 128, blk * 128 : blk * 128 + 128] = fro

    chosen = one_where(iota((256, EDGES), 0).astype(F32) == jnp.broadcast_to(turns, (256, EDGES)))
    whole = wig_ref[...]
    first = whole.astype(BF16)
    rest = whole - first.astype(F32)
    second = rest.astype(BF16)
    third = (rest - second.astype(F32)).astype(BF16)
    wige[...] = dot(first, chosen) + (dot(second, chosen) + dot(third, chosen))

    def keep_p(pos, value):
        ps[pos] = value

    rotate_in(dot(to_rows(g_ref, pad).astype(BF16), gat_tile[...]), wige, feats, keep_p)

    for lev in range(7):
        tile = w0_ref[:, lev].reshape(112, 128).astype(F32)
        wt0[lev * 128 : lev * 128 + 128, :] = (
            jnp.concatenate([tile, jnp.zeros((16, 128), F32)], 0).T.astype(BF16)
        )
    for ref, out, n in ((w1_ref, wt1, 6), (w2_ref, wt2, 5)):
        for part in range(2):
            for lev in range(n):
                tile = ref[part, :, lev].reshape(n * 16, 128).astype(F32)
                tile = jnp.concatenate([tile, jnp.zeros((128 - n * 16, 128), F32)], 0)
                out[lev * 128 : lev * 128 + 128, part * 128 : part * 128 + 128] = (
                    tile.T.astype(BF16)
                )
    back[...] = jnp.zeros_like(back)

    near = [zh * 4 + lax.rem(xi + off, 4) for off in (1, 3, 2)]
    far = [(1 - zh) * 4 + lax.rem(xi + off, 4) for off in (1, 3, 2)]
    mirror = lax.rem(ch + 4, 8)
    arrival(0, near[0])
    go(1, near[0], up)
    go(2, near[0], down)
    arrival(0, near[1])
    go(1, near[1], up)
    go(2, near[1], down)
    arrival(0, near[2])
    go(1, near[2], up)
    go(2, near[2], down)
    arrival(0, mirror)
    for off in (2, 1, 3):
        go(0, mirror, peer(off))
    go(1, mirror, up)
    go(2, mirror, down)
    for who in far:
        arrival(0, who)
        go(1, who, up)
        go(2, who, down)

    def chunk_in(i, carry):
        side = lax.rem(zh + i // 4, 2)
        who = side * 4 + lax.rem(xi + lax.rem(i, 4), 4)
        arrival(1, who)
        arrival(2, who)
        lhs = jnp.concatenate([tab[0, who], tab[1, who], tab[2, who]], 1)

        def keep(pos, value):
            rot[pl.ds(pl.multiple_of(pos * 128 + who * 16, 16), 16), :] = value.astype(BF16)

        rotate_in(dot(lhs, gat[...]), wige, feats, keep)
        return carry

    lax.fori_loop(0, 8, chunk_in, 0)
    for copy in sends:
        copy.wait_send()

    w0 = jnp.concatenate([w0_ref[:, lev].reshape(112, 128) for lev in range(7)], 1)
    y0 = dot(w0, rot[0:896, :])
    ys[0:7] = y0.reshape(7, 16, EDGES)
    for ref, n, start in ((w1_ref, 6, 7), (w2_ref, 5, 19)):
        lhs = jnp.concatenate(
            [ref[:, :, lev].reshape(2 * n * 16, 128) for lev in range(n)], 1
        )
        plus = rot[start * 128 : (start + n) * 128, :]
        minus = rot[(start + n) * 128 : (start + 2 * n) * 128, :]
        both = dot(lhs, jnp.concatenate([plus, minus], 1))
        half = n * 16
        ys[start : start + n] = (both[:half, :128] - both[half:, 128:]).reshape(n, 16, EDGES)
        ys[start + n : start + 2 * n] = (both[:half, 128:] + both[half:, :128]).reshape(
            n, 16, EDGES
        )

    attn = jnp.zeros((16, EDGES), F32)
    rows = iota((16, EDGES), 0)
    for t in range(16):
        attn = jnp.where(rows == t, attn_ref[t], attn)
    scalar = ys[0]
    gate = jax.nn.sigmoid(scalar)
    score = jnp.sum(scalar * gate * attn, axis=0, keepdims=True)
    live = jnp.broadcast_to((lane // 16) < count, (8, EDGES))
    score = jnp.broadcast_to(score, (8, EDGES))
    masked = jnp.where(live, score, -1e30)
    top = masked
    for shift in (16, 32, 64):
        top = jnp.maximum(top, spin(top, shift))
    weight = jnp.exp(jnp.where(live, score - top, -1e30))
    total = weight
    for shift in (16, 32, 64):
        total = total + spin(total, shift)
    weight = weight / total
    weight2 = jnp.concatenate([weight, weight], 0)
    inner = ys[0] * ps[0]
    for pos in range(1, 29):
        inner = inner + ys[pos] * ps[pos]
    dweight = jnp.broadcast_to(jnp.sum(inner * gate, axis=0, keepdims=True), (8, EDGES))
    mean = weight * dweight
    for shift in (16, 32, 64):
        mean = mean + spin(mean, shift)
    dscore = weight * (dweight - mean)
    dscore2 = jnp.concatenate([dscore, dscore], 0)
    slope = gate * (1.0 - gate)
    dscalar = weight2 * inner * slope + dscore2 * attn * (gate + scalar * slope)
    factor = weight2 * gate

    nil = jnp.zeros((16, EDGES), F32)
    dys = [ps[pos] * factor for pos in range(29)]
    dys[0] = dys[0] + dscalar
    dy0 = jnp.concatenate(dys[0:7] + [nil], 0).astype(BF16)
    drot[0:896, :] = dot(wt0[...], dy0).astype(BF16)
    for out, n, start in ((wt1, 6, 7), (wt2, 5, 19)):
        plus = jnp.concatenate(dys[start : start + n] + [nil] * (8 - n), 0).astype(BF16)
        minus = jnp.concatenate(dys[start + n : start + 2 * n] + [nil] * (8 - n), 0).astype(BF16)
        rhs = jnp.concatenate(
            [jnp.concatenate([plus, minus], 1), jnp.concatenate([minus, -plus], 1)], 0
        )
        both = dot(out[...], rhs)
        drot[start * 128 : (start + n) * 128, :] = both[:, :128].astype(BF16)
        drot[(start + n) * 128 : (start + 2 * n) * 128, :] = both[:, 128:].astype(BF16)

    def group_of(i):
        off = jnp.where(i < 2, 2, jnp.where(i < 4, 1, jnp.where(i < 6, 3, 0)))
        return lax.rem(i, 2) * 4 + lax.rem(xi + off, 4)

    def to_down(i):
        return rcopy(
            below_out.at[i], from_above.at[i], ghost_send.at[0, i], ghost_recv.at[0, i], down
        )

    def to_up(i):
        return rcopy(
            above_out.at[i], from_below.at[i], ghost_send.at[1, i], ghost_recv.at[1, i], up
        )

    def chunk_out(i, carry):
        who = group_of(i)

        def read(pos):
            value = drot[pl.ds(pl.multiple_of(pos * 128 + who * 16, 16), 16), :].astype(F32)
            return value[0:8], value[8:16]

        rotate_out(read, wige, back)
        out = dot(across(back).astype(BF16), sca[...])
        accum[i] = out[:, 0:128]
        below_out[i] = out[:, 128:256].astype(BF16)
        above_out[i] = out[:, 256:384].astype(BF16)
        to_down(i).start()
        to_up(i).start()
        return carry

    lax.fori_loop(0, 8, chunk_out, 0)

    def to_peer(i, off):
        return rcopy(x_out.at[i], x_in.at[i], xs_send.at[i], xs_recv.at[i], peer(off))

    def finish(i):
        to_down(i).wait_recv()
        to_up(i).wait_recv()
        return accum[i] + from_above[i].astype(F32) + from_below[i].astype(F32)

    for i in range(6):
        x_out[i] = finish(i).astype(BF16)
        to_peer(i, (2, 2, 1, 1, 3, 3)[i]).start()
    for i in (6, 7):
        red[i - 6] = finish(i)

    def read_z(pos):
        value = ys[pos] * factor
        return value[0:8], value[8:16]

    rotate_out(read_z, wige, back)
    wide = across(back)
    first = wide.astype(BF16)
    second = (wide - first.astype(F32)).astype(BF16)
    agg = dot(first, sca_tile[...]) + dot(second, sca_tile[...])
    upd_ref[...] = (x_ref[...].astype(F32) + from_rows(agg)).astype(BF16)

    for i in range(6):
        to_peer(i, (2, 2, 1, 1, 3, 3)[i]).wait_recv()
        red[i % 2] = red[i % 2] + x_in[i].astype(F32)
    z_out[...] = red[1 - zh].astype(BF16)
    across_z = rcopy(z_out, z_in, zs_send.at[0], zs_recv.at[0], other)
    across_z.start()
    across_z.wait_recv()
    grad = red[zh] + z_in[...].astype(F32)
    grad_ref[...] = g_ref[...].astype(F32) + from_rows(grad)

    across_z.wait_send()
    for i in range(6):
        to_peer(i, (2, 2, 1, 1, 3, 3)[i]).wait_send()
    for i in range(8):
        to_down(i).wait_send()
        to_up(i).wait_send()


def on_device(
    node_irreps,
    out_grad,
    edge_source,
    edge_rotation,
    edge_count,
    ghost_slot,
    wigner,
    so2_m0,
    so2_m1,
    so2_m2,
    attn_vector,
):
    vmem = pl.BlockSpec(memory_space=pltpu.VMEM)
    smem = pl.BlockSpec(memory_space=pltpu.SMEM)
    block = (ROWS, 128)
    dma = pltpu.SemaphoreType.DMA
    upd, grad = pl.pallas_call(
        body,
        out_shape=(
            jax.ShapeDtypeStruct((16, 16, K), BF16),
            jax.ShapeDtypeStruct((16, 16, K), F32),
        ),
        in_specs=[vmem, vmem, vmem, vmem, smem, smem, vmem, vmem, vmem, vmem, smem],
        out_specs=(vmem, vmem),
        scratch_shapes=[
            pltpu.VMEM((3, 8) + block, BF16),
            pltpu.VMEM((256, 128), F32),
            pltpu.VMEM((455, EDGES), F32),
            pltpu.VMEM((384, 1024), BF16),
            pltpu.VMEM((1024, 384), BF16),
            pltpu.VMEM((128, 1024), BF16),
            pltpu.VMEM((1024, 128), BF16),
            pltpu.VMEM((8 * PITCH, 128), F32),
            pltpu.VMEM((8 * PITCH, 128), F32),
            pltpu.VMEM((29 * 128, EDGES), BF16),
            pltpu.VMEM((29 * 128, EDGES), BF16),
            pltpu.VMEM((29, 16, EDGES), F32),
            pltpu.VMEM((29, 16, EDGES), F32),
            pltpu.VMEM((896, 128), BF16),
            pltpu.VMEM((768, 256), BF16),
            pltpu.VMEM((640, 256), BF16),
            pltpu.VMEM((8,) + block, F32),
            pltpu.VMEM((8,) + block, BF16),
            pltpu.VMEM((8,) + block, BF16),
            pltpu.VMEM((8,) + block, BF16),
            pltpu.VMEM((8,) + block, BF16),
            pltpu.VMEM((6,) + block, BF16),
            pltpu.VMEM((6,) + block, BF16),
            pltpu.VMEM(block, BF16),
            pltpu.VMEM(block, BF16),
            pltpu.VMEM((2,) + block, F32),
            dma((25,)),
            dma((3, 8)),
            dma((2, 8)),
            dma((2, 8)),
            dma((6,)),
            dma((6,)),
            dma((1,)),
            dma((1,)),
        ],
        compiler_params=pltpu.CompilerParams(
            collective_id=0, has_side_effects=True, vmem_limit_bytes=56 * 1024 * 1024
        ),
        name="layer",
    )(
        jnp.transpose(node_irreps, (1, 2, 0)),
        jnp.transpose(out_grad, (1, 2, 0)),
        edge_source,
        edge_rotation,
        edge_count,
        ghost_slot,
        wigner,
        jnp.transpose(so2_m0, (0, 2, 1, 3)),
        jnp.transpose(so2_m1, (0, 1, 3, 2, 4)),
        jnp.transpose(so2_m2, (0, 1, 3, 2, 4)),
        attn_vector,
    )
    return jnp.transpose(upd, (2, 0, 1)), jnp.transpose(grad, (2, 0, 1))


def solution(mesh):
    placed = (
        P(None, "ch", "dom"),
        P(None, "ch", "dom"),
        P(None, "dom"),
        P(None, "dom"),
        P("dom"),
        P("dom"),
        P(None, "dom"),
        P(None, "ch", None, None),
        P(None, None, "ch", None, None),
        P(None, None, "ch", None, None),
        P("ch"),
    )
    return jax.shard_map(
        on_device,
        mesh=mesh,
        in_specs=placed,
        out_specs=(P(None, "ch", "dom"), P(None, "ch", "dom")),
        check_vma=False,
    )
```

```python
import jax
import jax.numpy as jnp
from jax import lax
from jax.experimental import pallas as pl
from jax.experimental.pallas import tpu as pltpu
from jax.sharding import PartitionSpec as P

LMAX = 6
MMAX = 2
K = 49
OWN = 16
EDGES = 128
KP = 56
ROWS = 2 * KP
PITCH = 116
F32 = jnp.float32
BF16 = jnp.bfloat16
MESH = pl.DeviceIdType.MESH


def rows_of_levels():
    levels = []
    offset = 0
    for level in range(LMAX + 1):
        width = 2 * level + 1
        reach = min(level, MMAX)
        orders = list(range(-reach, reach + 1))
        levels.append((level, width, offset, orders))
        offset += width * width
    return levels


LEVELS = rows_of_levels()


def place(level, order):
    if order == 0:
        return level
    if order == 1:
        return 6 + level
    if order == -1:
        return 12 + level
    if order == 2:
        return 17 + level
    return 22 + level


def iota(shape, dim):
    return lax.broadcasted_iota(jnp.int32, shape, dim)


def one_where(cond):
    return jnp.where(cond, 1.0, 0.0).astype(BF16)


def spin(x, shift):
    return pltpu.roll(x, shift, 1)


def dot(a, b):
    return jnp.dot(a, b, preferred_element_type=F32)


def turn(wige, level, width, offset, order, col):
    row = offset + (level + order) * width + col
    return jnp.broadcast_to(wige[row : row + 1, :], (8, EDGES))


def rotate_in(mixed, wige, feats, write):
    for c in range(8):
        feats[c * PITCH : c * PITCH + ROWS, :] = mixed[:, c * EDGES : (c + 1) * EDGES]
    for level, width, offset, orders in LEVELS:
        acc = {}
        for col in range(width):
            k = level * level + col
            low = feats[pl.ds(k, 8, stride=PITCH), :]
            high = feats[pl.ds(KP + k, 8, stride=PITCH), :]
            for order in orders:
                w = turn(wige, level, width, offset, order, col)
                if col == 0:
                    acc[order] = (w * low, w * high)
                else:
                    a, b = acc[order]
                    acc[order] = (a + w * low, b + w * high)
        for order in orders:
            write(place(level, order), jnp.concatenate(acc[order], 0))


def rotate_out(read, wige, back):
    for level, width, offset, orders in LEVELS:
        mine = {order: read(place(level, order)) for order in orders}
        for col in range(width):
            k = level * level + col
            low = high = None
            for order in orders:
                w = turn(wige, level, width, offset, order, col)
                a, b = mine[order]
                low = w * a if low is None else low + w * a
                high = w * b if high is None else high + w * b
            back[pl.ds(k, 8, stride=PITCH), :] = low
            back[pl.ds(KP + k, 8, stride=PITCH), :] = high


def across(back):
    return jnp.concatenate([back[c * PITCH : c * PITCH + ROWS, :] for c in range(8)], 1)


def to_rows(ref, pad):
    pad[...] = jnp.zeros_like(pad)
    pad[:, 0:K] = ref[...].astype(F32).reshape(256, K)
    low = pad[0:128, :].T
    high = pad[128:256, :].T
    return jnp.concatenate([low[0:KP], high[0:KP]], 0)


def from_rows(rows):
    fill = jnp.zeros((128 - KP, 128), F32)
    low = jnp.concatenate([rows[0:KP], fill], 0).T
    high = jnp.concatenate([rows[KP:ROWS], fill], 0).T
    return jnp.concatenate([low, high], 0)[:, 0:K].reshape(16, 16, K)


def body(
    x_hbm,
    g_hbm,
    src_hbm,
    turn_hbm,
    cnt_hbm,
    slot_hbm,
    wig_hbm,
    w0_hbm,
    w1_hbm,
    w2_hbm,
    attn_hbm,
    upd_ref,
    grad_ref,
    x_ref,
    g_ref,
    src_ref,
    turn_ref,
    cnt_ref,
    slot_ref,
    wig_ref,
    w0_ref,
    w1_ref,
    w2_ref,
    attn_ref,
    load_sem,
    tab,
    pad,
    wige,
    gat,
    sca,
    gat_tile,
    sca_tile,
    feats,
    back,
    rot,
    drot,
    ys,
    ps,
    wt0,
    wt1,
    wt2,
    accum,
    below_out,
    above_out,
    from_above,
    from_below,
    x_out,
    x_in,
    z_out,
    z_in,
    red,
    send_sem,
    tab_sem,
    ghost_send,
    ghost_recv,
    xs_send,
    xs_recv,
    zs_send,
    zs_recv,
):
    doms = lax.axis_size("dom")
    d = lax.axis_index("dom")
    ch = lax.axis_index("ch")
    zh = ch // 4
    xi = lax.rem(ch, 4)
    up = (lax.rem(d + 1, doms), ch)
    down = (lax.rem(d + doms - 1, doms), ch)
    other = (d, lax.rem(ch + 4, 8))

    def peer(off):
        return (d, zh * 4 + lax.rem(xi + off, 4))

    barrier = pltpu.get_barrier_semaphore()
    for target in (up, down, other, peer(1), peer(2), peer(3)):
        pl.semaphore_signal(barrier, inc=1, device_id=target, device_id_type=MESH)

    loads = [
        pltpu.make_async_copy(src, dst, load_sem.at[n])
        for n, (src, dst) in enumerate(
            (
                (x_hbm, x_ref),
                (src_hbm, src_ref),
                (turn_hbm, turn_ref),
                (cnt_hbm, cnt_ref),
                (slot_hbm, slot_ref),
                (wig_hbm, wig_ref),
                (g_hbm, g_ref),
                (w0_hbm, w0_ref),
                (w1_hbm, w1_ref),
                (w2_hbm, w2_ref),
                (attn_hbm, attn_ref),
            )
        )
    ]
    for load in loads:
        load.start()
    loads[0].wait()
    tab[0, ch] = to_rows(x_ref, pad).astype(BF16)

    def rcopy(src, dst, ssem, rsem, target):
        return pltpu.make_async_remote_copy(
            src_ref=src,
            dst_ref=dst,
            send_sem=ssem,
            recv_sem=rsem,
            device_id=target,
            device_id_type=MESH,
        )

    def table_copy(blk, who, n, target):
        return rcopy(
            tab.at[0, who], tab.at[blk, who], send_sem.at[n], tab_sem.at[blk, who], target
        )

    def arrival(blk, who):
        return rcopy(
            tab.at[0, who], tab.at[blk, who], send_sem.at[0], tab_sem.at[blk, who], up
        ).wait_recv()

    pl.semaphore_wait(barrier, 6)
    sends = []

    def go(blk, who, target):
        copy = table_copy(blk, who, len(sends), target)
        copy.start()
        sends.append(copy)

    go(0, ch, other)
    for off in (2, 1, 3):
        go(0, ch, peer(off))
    go(1, ch, up)
    go(2, ch, down)

    for load in loads[1:6]:
        load.wait()

    spread = one_where(lax.rem(iota((16, EDGES), 1), 16) == iota((16, EDGES), 0))
    pick = (iota((8, EDGES), 1) // 16) == iota((8, EDGES), 0)

    def edge_row(ref):
        wide = dot(ref[...].astype(F32).astype(BF16), spread)
        return jnp.sum(jnp.where(pick, wide, 0.0), axis=0, keepdims=True)

    src = edge_row(src_ref)
    turns = edge_row(turn_ref)
    lane = iota((1, EDGES), 1)
    atom = lax.rem(lane, 16)
    ghost = jnp.zeros((1, EDGES), F32)
    count = jnp.zeros((1, EDGES), jnp.int32)
    for a in range(16):
        ghost = jnp.where(src == 16.0 + a, slot_ref[a].astype(F32), ghost)
        count = jnp.where(atom == a, cnt_ref[a], count)
    nowhere = -1000.0
    index = (
        jnp.where(src < 16.0, src, nowhere),
        jnp.where((src >= 16.0) & (src < 24.0), ghost, nowhere),
        jnp.where(src >= 24.0, ghost, nowhere),
    )
    row_id = iota((EDGES, EDGES), 0).astype(F32)
    lane_id = iota((EDGES, EDGES), 1).astype(F32)
    for blk in range(4):
        idx = atom.astype(F32) if blk == 3 else index[blk]
        wide = jnp.broadcast_to(idx, (EDGES, EDGES))
        tall = wide.T
        for c in range(8):
            forth = one_where(row_id == wide + 16.0 * c)
            fro = one_where(lane_id == tall + 16.0 * c)
            if blk == 3:
                gat_tile[:, c * 128 : c * 128 + 128] = forth
                sca_tile[c * 128 : c * 128 + 128, :] = fro
            else:
                gat[blk * 128 : blk * 128 + 128, c * 128 : c * 128 + 128] = forth
                sca[c * 128 : c * 128 + 128, blk * 128 : blk * 128 + 128] = fro

    chosen = one_where(iota((256, EDGES), 0).astype(F32) == jnp.broadcast_to(turns, (256, EDGES)))
    whole = wig_ref[...]
    first = whole.astype(BF16)
    rest = whole - first.astype(F32)
    second = rest.astype(BF16)
    third = (rest - second.astype(F32)).astype(BF16)
    wige[...] = dot(first, chosen) + (dot(second, chosen) + dot(third, chosen))

    for load in loads[6:]:
        load.wait()

    def keep_p(pos, value):
        ps[pos] = value

    rotate_in(dot(to_rows(g_ref, pad).astype(BF16), gat_tile[...]), wige, feats, keep_p)

    for lev in range(7):
        tile = w0_ref[:, lev].reshape(112, 128).astype(F32)
        wt0[lev * 128 : lev * 128 + 128, :] = (
            jnp.concatenate([tile, jnp.zeros((16, 128), F32)], 0).T.astype(BF16)
        )
    for ref, out, n in ((w1_ref, wt1, 6), (w2_ref, wt2, 5)):
        for part in range(2):
            for lev in range(n):
                tile = ref[part, :, lev].reshape(n * 16, 128).astype(F32)
                tile = jnp.concatenate([tile, jnp.zeros((128 - n * 16, 128), F32)], 0)
                out[lev * 128 : lev * 128 + 128, part * 128 : part * 128 + 128] = (
                    tile.T.astype(BF16)
                )
    back[...] = jnp.zeros_like(back)

    near = [zh * 4 + lax.rem(xi + off, 4) for off in (1, 3, 2)]
    far = [(1 - zh) * 4 + lax.rem(xi + off, 4) for off in (1, 3, 2)]
    mirror = lax.rem(ch + 4, 8)
    arrival(0, near[0])
    go(1, near[0], up)
    go(2, near[0], down)
    arrival(0, near[1])
    go(1, near[1], up)
    go(2, near[1], down)
    arrival(0, near[2])
    go(1, near[2], up)
    go(2, near[2], down)
    arrival(0, mirror)
    for off in (2, 1, 3):
        go(0, mirror, peer(off))
    go(1, mirror, up)
    go(2, mirror, down)
    for who in far:
        arrival(0, who)
        go(1, who, up)
        go(2, who, down)

    def chunk_in(i, carry):
        side = lax.rem(zh + i // 4, 2)
        who = side * 4 + lax.rem(xi + lax.rem(i, 4), 4)
        arrival(1, who)
        arrival(2, who)
        lhs = jnp.concatenate([tab[0, who], tab[1, who], tab[2, who]], 1)

        def keep(pos, value):
            rot[pl.ds(pl.multiple_of(pos * 128 + who * 16, 16), 16), :] = value.astype(BF16)

        rotate_in(dot(lhs, gat[...]), wige, feats, keep)
        return carry

    lax.fori_loop(0, 8, chunk_in, 0)
    for copy in sends:
        copy.wait_send()

    w0 = jnp.concatenate([w0_ref[:, lev].reshape(112, 128) for lev in range(7)], 1)
    y0 = dot(w0, rot[0:896, :])
    ys[0:7] = y0.reshape(7, 16, EDGES)
    for ref, n, start in ((w1_ref, 6, 7), (w2_ref, 5, 19)):
        lhs = jnp.concatenate(
            [ref[:, :, lev].reshape(2 * n * 16, 128) for lev in range(n)], 1
        )
        plus = rot[start * 128 : (start + n) * 128, :]
        minus = rot[(start + n) * 128 : (start + 2 * n) * 128, :]
        both = dot(lhs, jnp.concatenate([plus, minus], 1))
        half = n * 16
        ys[start : start + n] = (both[:half, :128] - both[half:, 128:]).reshape(n, 16, EDGES)
        ys[start + n : start + 2 * n] = (both[:half, 128:] + both[half:, :128]).reshape(
            n, 16, EDGES
        )

    attn = jnp.zeros((16, EDGES), F32)
    rows = iota((16, EDGES), 0)
    for t in range(16):
        attn = jnp.where(rows == t, attn_ref[t], attn)
    scalar = ys[0]
    gate = jax.nn.sigmoid(scalar)
    score = jnp.sum(scalar * gate * attn, axis=0, keepdims=True)
    live = jnp.broadcast_to((lane // 16) < count, (8, EDGES))
    score = jnp.broadcast_to(score, (8, EDGES))
    masked = jnp.where(live, score, -1e30)
    top = masked
    for shift in (16, 32, 64):
        top = jnp.maximum(top, spin(top, shift))
    weight = jnp.exp(jnp.where(live, score - top, -1e30))
    total = weight
    for shift in (16, 32, 64):
        total = total + spin(total, shift)
    weight = weight / total
    weight2 = jnp.concatenate([weight, weight], 0)
    inner = ys[0] * ps[0]
    for pos in range(1, 29):
        inner = inner + ys[pos] * ps[pos]
    dweight = jnp.broadcast_to(jnp.sum(inner * gate, axis=0, keepdims=True), (8, EDGES))
    mean = weight * dweight
    for shift in (16, 32, 64):
        mean = mean + spin(mean, shift)
    dscore = weight * (dweight - mean)
    dscore2 = jnp.concatenate([dscore, dscore], 0)
    slope = gate * (1.0 - gate)
    dscalar = weight2 * inner * slope + dscore2 * attn * (gate + scalar * slope)
    factor = weight2 * gate

    nil = jnp.zeros((16, EDGES), F32)
    dys = [ps[pos] * factor for pos in range(29)]
    dys[0] = dys[0] + dscalar
    dy0 = jnp.concatenate(dys[0:7] + [nil], 0).astype(BF16)
    drot[0:896, :] = dot(wt0[...], dy0).astype(BF16)
    for out, n, start in ((wt1, 6, 7), (wt2, 5, 19)):
        plus = jnp.concatenate(dys[start : start + n] + [nil] * (8 - n), 0).astype(BF16)
        minus = jnp.concatenate(dys[start + n : start + 2 * n] + [nil] * (8 - n), 0).astype(BF16)
        rhs = jnp.concatenate(
            [jnp.concatenate([plus, minus], 1), jnp.concatenate([minus, -plus], 1)], 0
        )
        both = dot(out[...], rhs)
        drot[start * 128 : (start + n) * 128, :] = both[:, :128].astype(BF16)
        drot[(start + n) * 128 : (start + 2 * n) * 128, :] = both[:, 128:].astype(BF16)

    def group_of(i):
        half = i // 4
        j = lax.rem(i, 4)
        off = jnp.where(j == 0, 2, jnp.where(j == 1, 1, jnp.where(j == 2, 3, 0)))
        return lax.rem(1 - zh + half, 2) * 4 + lax.rem(xi + off, 4)

    def to_down(i):
        return rcopy(
            below_out.at[i], from_above.at[i], ghost_send.at[0, i], ghost_recv.at[0, i], down
        )

    def to_up(i):
        return rcopy(
            above_out.at[i], from_below.at[i], ghost_send.at[1, i], ghost_recv.at[1, i], up
        )

    def chunk_out(i, carry):
        who = group_of(i)

        def read(pos):
            value = drot[pl.ds(pl.multiple_of(pos * 128 + who * 16, 16), 16), :].astype(F32)
            return value[0:8], value[8:16]

        rotate_out(read, wige, back)
        out = dot(across(back).astype(BF16), sca[...])
        accum[i] = out[:, 0:128]
        below_out[i] = out[:, 128:256].astype(BF16)
        above_out[i] = out[:, 256:384].astype(BF16)
        to_down(i).start()
        to_up(i).start()
        return carry

    lax.fori_loop(0, 8, chunk_out, 0)

    def to_peer(i, off):
        return rcopy(x_out.at[i], x_in.at[i], xs_send.at[i], xs_recv.at[i], peer(off))

    def finish(i):
        to_down(i).wait_recv()
        to_up(i).wait_recv()
        return accum[i] + from_above[i].astype(F32) + from_below[i].astype(F32)

    offs = (2, 1, 3)
    for half in range(2):
        for j in range(3):
            x_out[half * 3 + j] = finish(half * 4 + j).astype(BF16)
            to_peer(half * 3 + j, offs[j]).start()
        red[half] = finish(half * 4 + 3)

    def gathered(half):
        total = red[half]
        for j in range(3):
            to_peer(half * 3 + j, offs[j]).wait_recv()
            total = total + x_in[half * 3 + j].astype(F32)
        return total

    z_out[...] = gathered(0).astype(BF16)
    across_z = rcopy(z_out, z_in, zs_send.at[0], zs_recv.at[0], other)
    across_z.start()

    def read_z(pos):
        value = ys[pos] * factor
        return value[0:8], value[8:16]

    rotate_out(read_z, wige, back)
    wide = across(back)
    first = wide.astype(BF16)
    second = (wide - first.astype(F32)).astype(BF16)
    agg = dot(first, sca_tile[...]) + dot(second, sca_tile[...])
    upd_ref[...] = from_rows(agg)

    kept = gathered(1)
    across_z.wait_recv()
    grad = kept + z_in[...].astype(F32)
    grad_ref[...] = from_rows(grad)

    across_z.wait_send()
    for i in range(6):
        to_peer(i, offs[i % 3]).wait_send()
    for i in range(8):
        to_down(i).wait_send()
        to_up(i).wait_send()


def on_device(
    node_irreps,
    out_grad,
    edge_source,
    edge_rotation,
    edge_count,
    ghost_slot,
    wigner,
    so2_m0,
    so2_m1,
    so2_m2,
    attn_vector,
):
    vmem = pl.BlockSpec(memory_space=pltpu.VMEM)
    hbm = pl.BlockSpec(memory_space=pltpu.HBM)
    block = (ROWS, 128)
    dma = pltpu.SemaphoreType.DMA
    upd, grad = pl.pallas_call(
        body,
        out_shape=(
            jax.ShapeDtypeStruct((16, 16, K), F32),
            jax.ShapeDtypeStruct((16, 16, K), F32),
        ),
        in_specs=[hbm] * 11,
        out_specs=(vmem, vmem),
        scratch_shapes=[
            pltpu.VMEM((16, 16, K), BF16),
            pltpu.VMEM((16, 16, K), BF16),
            pltpu.VMEM((8, 16), jnp.int32),
            pltpu.VMEM((8, 16), jnp.int32),
            pltpu.SMEM((16,), jnp.int32),
            pltpu.SMEM((16,), jnp.int32),
            pltpu.VMEM((455, 256), F32),
            pltpu.VMEM((7, 7, 16, 128), BF16),
            pltpu.VMEM((2, 6, 6, 16, 128), BF16),
            pltpu.VMEM((2, 5, 5, 16, 128), BF16),
            pltpu.SMEM((16,), F32),
            dma((11,)),
            pltpu.VMEM((3, 8) + block, BF16),
            pltpu.VMEM((256, 128), F32),
            pltpu.VMEM((455, EDGES), F32),
            pltpu.VMEM((384, 1024), BF16),
            pltpu.VMEM((1024, 384), BF16),
            pltpu.VMEM((128, 1024), BF16),
            pltpu.VMEM((1024, 128), BF16),
            pltpu.VMEM((8 * PITCH, 128), F32),
            pltpu.VMEM((8 * PITCH, 128), F32),
            pltpu.VMEM((29 * 128, EDGES), BF16),
            pltpu.VMEM((29 * 128, EDGES), BF16),
            pltpu.VMEM((29, 16, EDGES), F32),
            pltpu.VMEM((29, 16, EDGES), F32),
            pltpu.VMEM((896, 128), BF16),
            pltpu.VMEM((768, 256), BF16),
            pltpu.VMEM((640, 256), BF16),
            pltpu.VMEM((8,) + block, F32),
            pltpu.VMEM((8,) + block, BF16),
            pltpu.VMEM((8,) + block, BF16),
            pltpu.VMEM((8,) + block, BF16),
            pltpu.VMEM((8,) + block, BF16),
            pltpu.VMEM((6,) + block, BF16),
            pltpu.VMEM((6,) + block, BF16),
            pltpu.VMEM(block, BF16),
            pltpu.VMEM(block, BF16),
            pltpu.VMEM((2,) + block, F32),
            dma((25,)),
            dma((3, 8)),
            dma((2, 8)),
            dma((2, 8)),
            dma((6,)),
            dma((6,)),
            dma((1,)),
            dma((1,)),
        ],
        compiler_params=pltpu.CompilerParams(
            collective_id=0, has_side_effects=True, vmem_limit_bytes=24 * 1024 * 1024
        ),
        name="layer",
    )(
        *(
            pltpu.with_memory_space_constraint(array, pltpu.HBM)
            for array in (
                jnp.transpose(node_irreps, (1, 2, 0)),
                jnp.transpose(out_grad, (1, 2, 0)),
                edge_source,
                edge_rotation,
                edge_count,
                ghost_slot,
                wigner,
                jnp.transpose(so2_m0, (0, 2, 1, 3)),
                jnp.transpose(so2_m1, (0, 1, 3, 2, 4)),
                jnp.transpose(so2_m2, (0, 1, 3, 2, 4)),
                attn_vector,
            )
        )
    )
    updated = node_irreps.astype(F32) + jnp.transpose(upd, (2, 0, 1))
    irreps_grad = out_grad.astype(F32) + jnp.transpose(grad, (2, 0, 1))
    return updated.astype(BF16), irreps_grad


def solution(mesh):
    placed = (
        P(None, "ch", "dom"),
        P(None, "ch", "dom"),
        P(None, "dom"),
        P(None, "dom"),
        P("dom"),
        P("dom"),
        P(None, "dom"),
        P(None, "ch", None, None),
        P(None, None, "ch", None, None),
        P(None, None, "ch", None, None),
        P("ch"),
    )
    return jax.shard_map(
        on_device,
        mesh=mesh,
        in_specs=placed,
        out_specs=(P(None, "ch", "dom"), P(None, "ch", "dom")),
        check_vma=False,
    )
```

```python
import jax
import jax.numpy as jnp
from jax import lax
from jax.experimental import pallas as pl
from jax.experimental.pallas import tpu as pltpu
from jax.sharding import PartitionSpec as P

LMAX = 6
MMAX = 2
K = 49
OWN = 16
EDGES = 128
KP = 56
ROWS = 2 * KP
PITCH = 116
F32 = jnp.float32
BF16 = jnp.bfloat16
MESH = pl.DeviceIdType.MESH


def rows_of_levels():
    levels = []
    offset = 0
    for level in range(LMAX + 1):
        width = 2 * level + 1
        reach = min(level, MMAX)
        orders = list(range(-reach, reach + 1))
        levels.append((level, width, offset, orders))
        offset += width * width
    return levels


LEVELS = rows_of_levels()


def place(level, order):
    if order == 0:
        return level
    if order == 1:
        return 6 + level
    if order == -1:
        return 12 + level
    if order == 2:
        return 17 + level
    return 22 + level


def iota(shape, dim):
    return lax.broadcasted_iota(jnp.int32, shape, dim)


def one_where(cond):
    return jnp.where(cond, 1.0, 0.0).astype(BF16)


def spin(x, shift):
    return pltpu.roll(x, shift, 1)


def dot(a, b):
    return jnp.dot(a, b, preferred_element_type=F32)


def turn(wige, level, width, offset, order, col):
    row = offset + (level + order) * width + col
    return jnp.broadcast_to(wige[row : row + 1, :], (8, EDGES))


def rotate_in(mixed, wige, feats, write):
    groups = range(mixed.shape[0] // ROWS)
    for n in groups:
        for c in range(8):
            feats[n, c * PITCH : c * PITCH + ROWS, :] = mixed[
                n * ROWS : (n + 1) * ROWS, c * EDGES : (c + 1) * EDGES
            ]
    for level, width, offset, orders in LEVELS:
        acc = {}
        for col in range(width):
            k = level * level + col
            parts = [
                feats[n, pl.ds(start + k, 8, stride=PITCH), :] for n in groups for start in (0, KP)
            ]
            for order in orders:
                w = turn(wige, level, width, offset, order, col)
                if col == 0:
                    acc[order] = [w * part for part in parts]
                else:
                    acc[order] = [old + w * part for old, part in zip(acc[order], parts)]
        for order in orders:
            for n in groups:
                write(n, place(level, order), jnp.concatenate(acc[order][2 * n : 2 * n + 2], 0))


def rotate_out(read, wige, back, count):
    for level, width, offset, orders in LEVELS:
        mine = {
            order: [part for n in range(count) for part in read(n, place(level, order))]
            for order in orders
        }
        for col in range(width):
            k = level * level + col
            total = None
            for order in orders:
                w = turn(wige, level, width, offset, order, col)
                if total is None:
                    total = [w * part for part in mine[order]]
                else:
                    total = [old + w * part for old, part in zip(total, mine[order])]
            for n in range(count):
                back[n, pl.ds(k, 8, stride=PITCH), :] = total[2 * n]
                back[n, pl.ds(KP + k, 8, stride=PITCH), :] = total[2 * n + 1]


def across(back, count):
    return jnp.concatenate(
        [
            jnp.concatenate([back[n, c * PITCH : c * PITCH + ROWS, :] for c in range(8)], 1)
            for n in range(count)
        ],
        0,
    )


def to_rows(ref, pad):
    pad[...] = jnp.zeros_like(pad)
    pad[:, 0:K] = ref[...].astype(F32).reshape(256, K)
    low = pad[0:128, :].T
    high = pad[128:256, :].T
    return jnp.concatenate([low[0:KP], high[0:KP]], 0)


def from_rows(rows):
    fill = jnp.zeros((128 - KP, 128), F32)
    low = jnp.concatenate([rows[0:KP], fill], 0).T
    high = jnp.concatenate([rows[KP:ROWS], fill], 0).T
    return jnp.concatenate([low, high], 0)[:, 0:K].reshape(16, 16, K)


def body(
    x_hbm,
    g_hbm,
    src_hbm,
    turn_hbm,
    cnt_hbm,
    slot_hbm,
    wig_hbm,
    w0_hbm,
    w1_hbm,
    w2_hbm,
    attn_hbm,
    upd_ref,
    grad_ref,
    x_ref,
    g_ref,
    src_ref,
    turn_ref,
    cnt_ref,
    slot_ref,
    wig_ref,
    w0_ref,
    w1_ref,
    w2_ref,
    attn_ref,
    load_sem,
    tab,
    pad,
    wige,
    gat,
    sca,
    gat_tile,
    sca_tile,
    feats,
    back,
    rot,
    drot,
    ys,
    ps,
    wt0,
    wt1,
    wt2,
    accum,
    ghost_out,
    from_above,
    from_below,
    x_out,
    x_in,
    z_out,
    z_in,
    red,
    end_x,
    end_sum,
    end_got,
    send_sem,
    tab_sem,
    ghost_send,
    ghost_recv,
    xs_send,
    xs_recv,
    zs_send,
    zs_recv,
    end_send,
    end_recv,
    end_last,
):
    doms = lax.axis_size("dom")
    d = lax.axis_index("dom")
    ch = lax.axis_index("ch")
    zh = ch // 4
    xi = lax.rem(ch, 4)
    mirror = lax.rem(ch + 4, 8)
    up = (lax.rem(d + 1, doms), ch)
    down = (lax.rem(d + doms - 1, doms), ch)
    other = (d, mirror)

    def peer(off):
        return (d, zh * 4 + lax.rem(xi + off, 4))

    has_up = d != doms - 1
    has_down = d != 0
    end = jnp.logical_or(d == 0, d == doms - 1)
    first_end = (doms - 1 - d, ch)
    second_end = (doms - 1 - d, mirror)
    end_in = jnp.where(d == 0, 1, 2)
    end_out = jnp.where(d == 0, 2, 1)
    end_side = jnp.where(d == 0, 0, 1)

    barrier = pltpu.get_barrier_semaphore()

    def greet(target):
        pl.semaphore_signal(barrier, inc=1, device_id=target, device_id_type=MESH)

    for target in (other, peer(1), peer(2), peer(3)):
        greet(target)
    pl.when(has_up)(lambda: greet(up))
    pl.when(has_down)(lambda: greet(down))

    @pl.when(end)
    def _():
        greet(first_end)
        greet(second_end)

    loads = [
        pltpu.make_async_copy(src, dst, load_sem.at[n])
        for n, (src, dst) in enumerate(
            (
                (x_hbm, x_ref),
                (src_hbm, src_ref),
                (turn_hbm, turn_ref),
                (cnt_hbm, cnt_ref),
                (slot_hbm, slot_ref),
                (wig_hbm, wig_ref),
                (g_hbm, g_ref),
                (w0_hbm, w0_ref),
                (w1_hbm, w1_ref),
                (w2_hbm, w2_ref),
                (attn_hbm, attn_ref),
            )
        )
    ]
    for load in loads:
        load.start()
    loads[0].wait()
    tab[0, ch] = to_rows(x_ref, pad).astype(BF16)

    def rcopy(src, dst, ssem, rsem, target):
        return pltpu.make_async_remote_copy(
            src_ref=src,
            dst_ref=dst,
            send_sem=ssem,
            recv_sem=rsem,
            device_id=target,
            device_id_type=MESH,
        )

    def table_copy(blk, who, n, target):
        return rcopy(
            tab.at[0, who], tab.at[blk, who], send_sem.at[n], tab_sem.at[blk, who], target
        )

    def arrival(blk, who):
        return rcopy(
            tab.at[0, who], tab.at[blk, who], send_sem.at[0], tab_sem.at[blk, who], up
        ).wait_recv()

    pl.semaphore_wait(barrier, jnp.where(end, 7, 6))
    sends = []

    def go(blk, who, target, cond=None):
        copy = table_copy(blk, who, len(sends), target)
        if cond is None:
            copy.start()
        else:
            pl.when(cond)(lambda: copy.start())
        sends.append((copy, cond))

    def halo(who):
        go(1, who, up, has_up)
        go(2, who, down, has_down)

    go(0, ch, other)
    go(end_out, ch, second_end, end)
    go(end_out, ch, first_end, end)
    for off in (2, 1, 3):
        go(0, ch, peer(off))
    halo(ch)

    for load in loads[1:6]:
        load.wait()

    spread = one_where(lax.rem(iota((16, EDGES), 1), 16) == iota((16, EDGES), 0))
    pick = (iota((8, EDGES), 1) // 16) == iota((8, EDGES), 0)

    def edge_row(ref):
        wide = dot(ref[...].astype(F32).astype(BF16), spread)
        return jnp.sum(jnp.where(pick, wide, 0.0), axis=0, keepdims=True)

    src = edge_row(src_ref)
    turns = edge_row(turn_ref)
    lane = iota((1, EDGES), 1)
    atom = lax.rem(lane, 16)
    ghost = jnp.zeros((1, EDGES), F32)
    count = jnp.zeros((1, EDGES), jnp.int32)
    for a in range(16):
        ghost = jnp.where(src == 16.0 + a, slot_ref[a].astype(F32), ghost)
        count = jnp.where(atom == a, cnt_ref[a], count)
    nowhere = -1000.0
    index = (
        jnp.where(src < 16.0, src, nowhere),
        jnp.where((src >= 16.0) & (src < 24.0), ghost, nowhere),
        jnp.where(src >= 24.0, ghost, nowhere),
    )
    row_id = iota((EDGES, EDGES), 0).astype(F32)
    lane_id = iota((EDGES, EDGES), 1).astype(F32)
    for blk in range(4):
        idx = atom.astype(F32) if blk == 3 else index[blk]
        wide = jnp.broadcast_to(idx, (EDGES, EDGES))
        tall = wide.T
        for c in range(8):
            forth = one_where(row_id == wide + 16.0 * c)
            fro = one_where(lane_id == tall + 16.0 * c)
            if blk == 3:
                gat_tile[:, c * 128 : c * 128 + 128] = forth
                sca_tile[c * 128 : c * 128 + 128, :] = fro
            else:
                gat[blk * 128 : blk * 128 + 128, c * 128 : c * 128 + 128] = forth
                sca[c * 128 : c * 128 + 128, blk * 128 : blk * 128 + 128] = fro

    chosen = one_where(iota((256, EDGES), 0).astype(F32) == jnp.broadcast_to(turns, (256, EDGES)))
    whole = wig_ref[...]
    first = whole.astype(BF16)
    rest = whole - first.astype(F32)
    second = rest.astype(BF16)
    third = (rest - second.astype(F32)).astype(BF16)
    wige[...] = dot(first, chosen) + (dot(second, chosen) + dot(third, chosen))

    for load in loads[6:]:
        load.wait()

    def keep_p(n, pos, value):
        ps[pos] = value

    rotate_in(dot(to_rows(g_ref, pad).astype(BF16), gat_tile[...]), wige, feats, keep_p)

    for lev in range(7):
        tile = w0_ref[:, lev].reshape(112, 128).astype(F32)
        wt0[lev * 128 : lev * 128 + 128, :] = (
            jnp.concatenate([tile, jnp.zeros((16, 128), F32)], 0).T.astype(BF16)
        )
    for ref, out, n in ((w1_ref, wt1, 6), (w2_ref, wt2, 5)):
        for part in range(2):
            for lev in range(n):
                tile = ref[part, :, lev].reshape(n * 16, 128).astype(F32)
                tile = jnp.concatenate([tile, jnp.zeros((128 - n * 16, 128), F32)], 0)
                out[lev * 128 : lev * 128 + 128, part * 128 : part * 128 + 128] = (
                    tile.T.astype(BF16)
                )
    back[...] = jnp.zeros_like(back)

    near = [zh * 4 + lax.rem(xi + off, 4) for off in (1, 3, 2)]
    far = [(1 - zh) * 4 + lax.rem(xi + off, 4) for off in (1, 3, 2)]
    arrival(0, near[0])
    halo(near[0])
    arrival(0, near[1])
    halo(near[1])
    arrival(0, near[2])
    halo(near[2])

    def end_copy(n, who, target):
        return rcopy(
            tab.at[end_in, who],
            tab.at[end_in, who],
            end_send.at[n],
            tab_sem.at[end_in, who],
            target,
        )

    @pl.when(end)
    def _():
        for n, who in enumerate((mirror, ch)):
            end_copy(0, who, first_end).wait_recv()
            for j, off in enumerate((2, 1, 3)):
                end_copy(n * 3 + j, who, peer(off)).start()

    arrival(0, mirror)
    for off in (2, 1, 3):
        go(0, mirror, peer(off))
    halo(mirror)
    for who in far:
        arrival(0, who)
        halo(who)

    def halo_arrival(blk, who):
        came = jnp.logical_and(end, jnp.logical_and(lax.rem(who, 4) == xi, blk == end_in))
        pl.when(jnp.logical_not(came))(lambda: arrival(blk, who))

    def pair_in(i, carry):
        side = lax.rem(zh + i // 2, 2)
        both = [side * 4 + lax.rem(xi + lax.rem(2 * i, 4) + n, 4) for n in range(2)]
        for who in both:
            halo_arrival(1, who)
            halo_arrival(2, who)
        lhs = jnp.concatenate(
            [jnp.concatenate([tab[0, who], tab[1, who], tab[2, who]], 1) for who in both], 0
        )

        def keep(n, pos, value):
            rot[pl.ds(pl.multiple_of(pos * 128 + both[n] * 16, 16), 16), :] = value.astype(BF16)

        rotate_in(dot(lhs, gat[...]), wige, feats, keep)
        return carry

    lax.fori_loop(0, 4, pair_in, 0)
    for copy, cond in sends:
        if cond is None:
            copy.wait_send()
        else:
            pl.when(cond)(lambda copy=copy: copy.wait_send())

    @pl.when(end)
    def _():
        for n, who in enumerate((mirror, ch)):
            for j, off in enumerate((2, 1, 3)):
                end_copy(n * 3 + j, who, peer(off)).wait_send()

    w0 = jnp.concatenate([w0_ref[:, lev].reshape(112, 128) for lev in range(7)], 1)
    y0 = dot(w0, rot[0:896, :])
    ys[0:7] = y0.reshape(7, 16, EDGES)
    for ref, n, start in ((w1_ref, 6, 7), (w2_ref, 5, 19)):
        lhs = jnp.concatenate(
            [ref[:, :, lev].reshape(2 * n * 16, 128) for lev in range(n)], 1
        )
        plus = rot[start * 128 : (start + n) * 128, :]
        minus = rot[(start + n) * 128 : (start + 2 * n) * 128, :]
        both = dot(lhs, jnp.concatenate([plus, minus], 1))
        half = n * 16
        ys[start : start + n] = (both[:half, :128] - both[half:, 128:]).reshape(n, 16, EDGES)
        ys[start + n : start + 2 * n] = (both[:half, 128:] + both[half:, :128]).reshape(
            n, 16, EDGES
        )

    attn = jnp.zeros((16, EDGES), F32)
    rows = iota((16, EDGES), 0)
    for t in range(16):
        attn = jnp.where(rows == t, attn_ref[t], attn)
    scalar = ys[0]
    gate = jax.nn.sigmoid(scalar)
    score = jnp.sum(scalar * gate * attn, axis=0, keepdims=True)
    live = jnp.broadcast_to((lane // 16) < count, (8, EDGES))
    score = jnp.broadcast_to(score, (8, EDGES))
    masked = jnp.where(live, score, -1e30)
    top = masked
    for shift in (16, 32, 64):
        top = jnp.maximum(top, spin(top, shift))
    weight = jnp.exp(jnp.where(live, score - top, -1e30))
    total = weight
    for shift in (16, 32, 64):
        total = total + spin(total, shift)
    weight = weight / total
    weight2 = jnp.concatenate([weight, weight], 0)
    inner = ys[0] * ps[0]
    for pos in range(1, 29):
        inner = inner + ys[pos] * ps[pos]
    dweight = jnp.broadcast_to(jnp.sum(inner * gate, axis=0, keepdims=True), (8, EDGES))
    mean = weight * dweight
    for shift in (16, 32, 64):
        mean = mean + spin(mean, shift)
    dscore = weight * (dweight - mean)
    dscore2 = jnp.concatenate([dscore, dscore], 0)
    slope = gate * (1.0 - gate)
    dscalar = weight2 * inner * slope + dscore2 * attn * (gate + scalar * slope)
    factor = weight2 * gate

    nil = jnp.zeros((16, EDGES), F32)
    dys = [ps[pos] * factor for pos in range(29)]
    dys[0] = dys[0] + dscalar
    dy0 = jnp.concatenate(dys[0:7] + [nil], 0).astype(BF16)
    drot[0:896, :] = dot(wt0[...], dy0).astype(BF16)
    for out, n, start in ((wt1, 6, 7), (wt2, 5, 19)):
        plus = jnp.concatenate(dys[start : start + n] + [nil] * (8 - n), 0).astype(BF16)
        minus = jnp.concatenate(dys[start + n : start + 2 * n] + [nil] * (8 - n), 0).astype(BF16)
        rhs = jnp.concatenate(
            [jnp.concatenate([plus, minus], 1), jnp.concatenate([minus, -plus], 1)], 0
        )
        both = dot(out[...], rhs)
        drot[start * 128 : (start + n) * 128, :] = both[:, :128].astype(BF16)
        drot[(start + n) * 128 : (start + 2 * n) * 128, :] = both[:, 128:].astype(BF16)

    def group_of(i):
        half = i // 4
        j = lax.rem(i, 4)
        off = jnp.where(j == 0, 2, jnp.where(j == 1, 1, jnp.where(j == 2, 3, 0)))
        return lax.rem(1 - zh + half, 2) * 4 + lax.rem(xi + off, 4)

    def to_down(who):
        return rcopy(
            ghost_out.at[0, who],
            from_above.at[who],
            ghost_send.at[0, who],
            ghost_recv.at[0, who],
            down,
        )

    def to_up(who):
        return rcopy(
            ghost_out.at[1, who],
            from_below.at[who],
            ghost_send.at[1, who],
            ghost_recv.at[1, who],
            up,
        )

    def pair_out(i, carry):
        both = [group_of(2 * i + n) for n in range(2)]

        def read(n, pos):
            start = pl.multiple_of(pos * 128 + both[n] * 16, 16)
            value = drot[pl.ds(start, 16), :].astype(F32)
            return value[0:8], value[8:16]

        rotate_out(read, wige, back, 2)
        out = dot(across(back, 2).astype(BF16), sca[...])
        for n, who in enumerate(both):
            part = out[n * ROWS : (n + 1) * ROWS]
            ghost_out[0, who] = part[:, 128:256].astype(BF16)
            ghost_out[1, who] = part[:, 256:384].astype(BF16)
            pl.when(has_down)(lambda who=who: to_down(who).start())
            pl.when(has_up)(lambda who=who: to_up(who).start())
            accum[who] = part[:, 0:128]
        return carry

    @pl.when(d == doms - 1)
    def _():
        from_above[...] = jnp.zeros_like(from_above)

    @pl.when(d == 0)
    def _():
        from_below[...] = jnp.zeros_like(from_below)

    lax.fori_loop(0, 4, pair_out, 0)

    offs = (2, 1, 3)

    def end_peer(i):
        half = i // 3
        off = offs[i % 3]
        who = ((zh + 1 - half) % 2) * 4 + lax.rem(xi + off, 4)
        return rcopy(
            ghost_out.at[end_side, who], end_x.at[i], end_send.at[i], end_recv.at[i], peer(off)
        )

    def end_home(half):
        target = (second_end, first_end)[half]
        return rcopy(
            end_sum.at[half], end_got.at[half], end_last.at[half], end_last.at[2 + half], target
        )

    @pl.when(end)
    def _():
        for i in range(6):
            end_peer(i).start()

    def to_peer(i, off):
        return rcopy(x_out.at[i], x_in.at[i], xs_send.at[i], xs_recv.at[i], peer(off))

    def finish(i):
        who = group_of(i)
        pl.when(has_up)(lambda: to_down(who).wait_recv())
        pl.when(has_down)(lambda: to_up(who).wait_recv())
        return accum[who] + from_above[who].astype(F32) + from_below[who].astype(F32)

    for half in range(2):
        for j in range(3):
            x_out[half * 3 + j] = finish(half * 4 + j).astype(BF16)
            to_peer(half * 3 + j, offs[j]).start()
        red[half] = finish(half * 4 + 3)

    def gathered(half):
        total = red[half]
        for j in range(3):
            to_peer(half * 3 + j, offs[j]).wait_recv()
            total = total + x_in[half * 3 + j].astype(F32)
        return total

    @pl.when(end)
    def _():
        for half in range(2):
            who = ((zh + 1 - half) % 2) * 4 + xi
            total = ghost_out[end_side, who].astype(F32)
            for j in range(3):
                end_peer(half * 3 + j).wait_recv()
                total = total + end_x[half * 3 + j].astype(F32)
            end_sum[half] = total.astype(BF16)
            end_home(half).start()

    z_out[...] = gathered(0).astype(BF16)
    across_z = rcopy(z_out, z_in, zs_send.at[0], zs_recv.at[0], other)
    across_z.start()

    def read_z(n, pos):
        value = ys[pos] * factor
        return value[0:8], value[8:16]

    rotate_out(read_z, wige, back, 1)
    wide = across(back, 1)
    first = wide.astype(BF16)
    second = (wide - first.astype(F32)).astype(BF16)
    agg = dot(first, sca_tile[...]) + dot(second, sca_tile[...])
    upd_ref[...] = from_rows(agg)

    red[1] = gathered(1)

    @pl.when(end)
    def _():
        end_home(0).wait_recv()
        end_home(1).wait_recv()
        red[1] = red[1] + (end_got[0].astype(F32) + end_got[1].astype(F32))

    across_z.wait_recv()
    grad = red[1] + z_in[...].astype(F32)
    grad_ref[...] = from_rows(grad)

    across_z.wait_send()
    for i in range(6):
        to_peer(i, offs[i % 3]).wait_send()
    for i in range(8):
        pl.when(has_down)(lambda i=i: to_down(i).wait_send())
        pl.when(has_up)(lambda i=i: to_up(i).wait_send())

    @pl.when(end)
    def _():
        for i in range(6):
            end_peer(i).wait_send()
        end_home(0).wait_send()
        end_home(1).wait_send()


def on_device(
    node_irreps,
    out_grad,
    edge_source,
    edge_rotation,
    edge_count,
    ghost_slot,
    wigner,
    so2_m0,
    so2_m1,
    so2_m2,
    attn_vector,
):
    vmem = pl.BlockSpec(memory_space=pltpu.VMEM)
    hbm = pl.BlockSpec(memory_space=pltpu.HBM)
    block = (ROWS, 128)
    dma = pltpu.SemaphoreType.DMA
    upd, grad = pl.pallas_call(
        body,
        out_shape=(
            jax.ShapeDtypeStruct((16, 16, K), F32),
            jax.ShapeDtypeStruct((16, 16, K), F32),
        ),
        in_specs=[hbm] * 11,
        out_specs=(vmem, vmem),
        scratch_shapes=[
            pltpu.VMEM((16, 16, K), BF16),
            pltpu.VMEM((16, 16, K), BF16),
            pltpu.VMEM((8, 16), jnp.int32),
            pltpu.VMEM((8, 16), jnp.int32),
            pltpu.SMEM((16,), jnp.int32),
            pltpu.SMEM((16,), jnp.int32),
            pltpu.VMEM((455, 256), F32),
            pltpu.VMEM((7, 7, 16, 128), BF16),
            pltpu.VMEM((2, 6, 6, 16, 128), BF16),
            pltpu.VMEM((2, 5, 5, 16, 128), BF16),
            pltpu.SMEM((16,), F32),
            dma((11,)),
            pltpu.VMEM((3, 8) + block, BF16),
            pltpu.VMEM((256, 128), F32),
            pltpu.VMEM((455, EDGES), F32),
            pltpu.VMEM((384, 1024), BF16),
            pltpu.VMEM((1024, 384), BF16),
            pltpu.VMEM((128, 1024), BF16),
            pltpu.VMEM((1024, 128), BF16),
            pltpu.VMEM((2, 8 * PITCH, 128), F32),
            pltpu.VMEM((2, 8 * PITCH, 128), F32),
            pltpu.VMEM((29 * 128, EDGES), BF16),
            pltpu.VMEM((29 * 128, EDGES), BF16),
            pltpu.VMEM((29, 16, EDGES), F32),
            pltpu.VMEM((29, 16, EDGES), F32),
            pltpu.VMEM((896, 128), BF16),
            pltpu.VMEM((768, 256), BF16),
            pltpu.VMEM((640, 256), BF16),
            pltpu.VMEM((8,) + block, F32),
            pltpu.VMEM((2, 8) + block, BF16),
            pltpu.VMEM((8,) + block, BF16),
            pltpu.VMEM((8,) + block, BF16),
            pltpu.VMEM((6,) + block, BF16),
            pltpu.VMEM((6,) + block, BF16),
            pltpu.VMEM(block, BF16),
            pltpu.VMEM(block, BF16),
            pltpu.VMEM((2,) + block, F32),
            pltpu.VMEM((6,) + block, BF16),
            pltpu.VMEM((2,) + block, BF16),
            pltpu.VMEM((2,) + block, BF16),
            dma((27,)),
            dma((3, 8)),
            dma((2, 8)),
            dma((2, 8)),
            dma((6,)),
            dma((6,)),
            dma((1,)),
            dma((1,)),
            dma((6,)),
            dma((6,)),
            dma((4,)),
        ],
        compiler_params=pltpu.CompilerParams(
            collective_id=0, has_side_effects=True, vmem_limit_bytes=24 * 1024 * 1024
        ),
        name="layer",
    )(
        *(
            pltpu.with_memory_space_constraint(array, pltpu.HBM)
            for array in (
                jnp.transpose(node_irreps, (1, 2, 0)),
                jnp.transpose(out_grad, (1, 2, 0)),
                edge_source,
                edge_rotation,
                edge_count,
                ghost_slot,
                wigner,
                jnp.transpose(so2_m0, (0, 2, 1, 3)),
                jnp.transpose(so2_m1, (0, 1, 3, 2, 4)),
                jnp.transpose(so2_m2, (0, 1, 3, 2, 4)),
                attn_vector,
            )
        )
    )
    updated = node_irreps.astype(F32) + jnp.transpose(upd, (2, 0, 1))
    irreps_grad = out_grad.astype(F32) + jnp.transpose(grad, (2, 0, 1))
    return updated.astype(BF16), irreps_grad


def solution(mesh):
    placed = (
        P(None, "ch", "dom"),
        P(None, "ch", "dom"),
        P(None, "dom"),
        P(None, "dom"),
        P("dom"),
        P("dom"),
        P(None, "dom"),
        P(None, "ch", None, None),
        P(None, None, "ch", None, None),
        P(None, None, "ch", None, None),
        P("ch"),
    )
    return jax.shard_map(
        on_device,
        mesh=mesh,
        in_specs=placed,
        out_specs=(P(None, "ch", "dom"), P(None, "ch", "dom")),
        check_vma=False,
    )
```

```python
import jax
import jax.numpy as jnp
from jax import lax
from jax.experimental import pallas as pl
from jax.experimental.pallas import tpu as pltpu
from jax.sharding import PartitionSpec as P

LMAX = 6
MMAX = 2
K = 49
OWN = 16
EDGES = 128
KP = 56
ROWS = 2 * KP
PITCH = 116
F32 = jnp.float32
BF16 = jnp.bfloat16
MESH = pl.DeviceIdType.MESH


def rows_of_levels():
    levels = []
    offset = 0
    for level in range(LMAX + 1):
        width = 2 * level + 1
        reach = min(level, MMAX)
        orders = list(range(-reach, reach + 1))
        levels.append((level, width, offset, orders))
        offset += width * width
    return levels


LEVELS = rows_of_levels()


def place(level, order):
    if order == 0:
        return level
    if order == 1:
        return 6 + level
    if order == -1:
        return 12 + level
    if order == 2:
        return 17 + level
    return 22 + level


def iota(shape, dim):
    return lax.broadcasted_iota(jnp.int32, shape, dim)


def one_where(cond):
    return jnp.where(cond, 1.0, 0.0).astype(BF16)


def spin(x, shift):
    return pltpu.roll(x, shift, 1)


def over_slots(x, join):
    parts = [x] + [spin(x, shift) for shift in range(OWN, EDGES, OWN)]
    while len(parts) > 1:
        parts = [join(parts[i], parts[i + 1]) for i in range(0, len(parts), 2)]
    return parts[0]


def dot(a, b):
    return jnp.dot(a, b, preferred_element_type=F32)


def turn(wige, level, width, offset, order, col):
    row = offset + (level + order) * width + col
    return jnp.broadcast_to(wige[row : row + 1, :], (8, EDGES))


def rotate_in(mixed, wige, feats, write):
    groups = range(mixed.shape[0] // ROWS)
    for n in groups:
        for c in range(8):
            feats[n, c * PITCH : c * PITCH + ROWS, :] = mixed[
                n * ROWS : (n + 1) * ROWS, c * EDGES : (c + 1) * EDGES
            ]
    for level, width, offset, orders in LEVELS:
        acc = {}
        for col in range(width):
            k = level * level + col
            parts = [
                feats[n, pl.ds(start + k, 8, stride=PITCH), :] for n in groups for start in (0, KP)
            ]
            for order in orders:
                w = turn(wige, level, width, offset, order, col)
                if col == 0:
                    acc[order] = [w * part for part in parts]
                else:
                    acc[order] = [old + w * part for old, part in zip(acc[order], parts)]
        for order in orders:
            for n in groups:
                write(n, place(level, order), jnp.concatenate(acc[order][2 * n : 2 * n + 2], 0))


def rotate_out(read, wige, back, count):
    for level, width, offset, orders in LEVELS:
        mine = {
            order: [part for n in range(count) for part in read(n, place(level, order))]
            for order in orders
        }
        for col in range(width):
            k = level * level + col
            total = None
            for order in orders:
                w = turn(wige, level, width, offset, order, col)
                if total is None:
                    total = [w * part for part in mine[order]]
                else:
                    total = [old + w * part for old, part in zip(total, mine[order])]
            for n in range(count):
                back[n, pl.ds(k, 8, stride=PITCH), :] = total[2 * n]
                back[n, pl.ds(KP + k, 8, stride=PITCH), :] = total[2 * n + 1]


def across(back, count):
    return jnp.concatenate(
        [
            jnp.concatenate([back[n, c * PITCH : c * PITCH + ROWS, :] for c in range(8)], 1)
            for n in range(count)
        ],
        0,
    )


def to_rows(ref, pad):
    pad[...] = jnp.zeros_like(pad)
    pad[:, 0:K] = ref[...].astype(F32).reshape(256, K)
    low = pad[0:128, :].T
    high = pad[128:256, :].T
    return jnp.concatenate([low[0:KP], high[0:KP]], 0)


def from_rows(rows):
    fill = jnp.zeros((128 - KP, 128), F32)
    low = jnp.concatenate([rows[0:KP], fill], 0).T
    high = jnp.concatenate([rows[KP:ROWS], fill], 0).T
    return jnp.concatenate([low, high], 0)[:, 0:K].reshape(16, 16, K)


def body(
    x_hbm,
    g_hbm,
    src_hbm,
    turn_hbm,
    cnt_hbm,
    slot_hbm,
    wig_hbm,
    w0_hbm,
    w1_hbm,
    w2_hbm,
    attn_hbm,
    upd_ref,
    grad_ref,
    x_ref,
    g_ref,
    src_ref,
    turn_ref,
    cnt_ref,
    slot_ref,
    wig_ref,
    w0_ref,
    w1_ref,
    w2_ref,
    attn_ref,
    load_sem,
    tab,
    pad,
    wige,
    gat,
    sca,
    gat_tile,
    sca_tile,
    feats,
    back,
    rot,
    drot,
    ys,
    ps,
    wt0,
    wt1,
    wt2,
    accum,
    ghost_out,
    from_above,
    from_below,
    x_out,
    x_in,
    z_out,
    z_in,
    red,
    end_x,
    end_sum,
    end_got,
    send_sem,
    tab_sem,
    ghost_send,
    ghost_recv,
    xs_send,
    xs_recv,
    zs_send,
    zs_recv,
    end_send,
    end_recv,
    end_last,
):
    doms = lax.axis_size("dom")
    d = lax.axis_index("dom")
    ch = lax.axis_index("ch")
    zh = ch // 4
    xi = lax.rem(ch, 4)
    mirror = lax.rem(ch + 4, 8)
    up = (lax.rem(d + 1, doms), ch)
    down = (lax.rem(d + doms - 1, doms), ch)
    other = (d, mirror)

    def peer(off):
        return (d, zh * 4 + lax.rem(xi + off, 4))

    has_up = d != doms - 1
    has_down = d != 0
    end = jnp.logical_or(d == 0, d == doms - 1)
    first_end = (doms - 1 - d, ch)
    second_end = (doms - 1 - d, mirror)
    end_in = jnp.where(d == 0, 1, 2)
    end_out = jnp.where(d == 0, 2, 1)
    end_side = jnp.where(d == 0, 0, 1)

    barrier = pltpu.get_barrier_semaphore()

    def greet(target):
        pl.semaphore_signal(barrier, inc=1, device_id=target, device_id_type=MESH)

    for target in (other, peer(1), peer(2), peer(3)):
        greet(target)
    pl.when(has_up)(lambda: greet(up))
    pl.when(has_down)(lambda: greet(down))

    @pl.when(end)
    def _():
        greet(first_end)
        greet(second_end)

    loads = [
        pltpu.make_async_copy(src, dst, load_sem.at[n])
        for n, (src, dst) in enumerate(
            (
                (x_hbm, x_ref),
                (src_hbm, src_ref),
                (turn_hbm, turn_ref),
                (cnt_hbm, cnt_ref),
                (slot_hbm, slot_ref),
                (wig_hbm, wig_ref),
                (g_hbm, g_ref),
                (w0_hbm, w0_ref),
                (w1_hbm, w1_ref),
                (w2_hbm, w2_ref),
                (attn_hbm, attn_ref),
            )
        )
    ]
    for load in loads:
        load.start()
    loads[0].wait()
    tab[0, ch] = to_rows(x_ref, pad).astype(BF16)

    def rcopy(src, dst, ssem, rsem, target):
        return pltpu.make_async_remote_copy(
            src_ref=src,
            dst_ref=dst,
            send_sem=ssem,
            recv_sem=rsem,
            device_id=target,
            device_id_type=MESH,
        )

    def table_copy(blk, who, n, target):
        return rcopy(
            tab.at[0, who], tab.at[blk, who], send_sem.at[n], tab_sem.at[blk, who], target
        )

    def arrival(blk, who):
        return rcopy(
            tab.at[0, who], tab.at[blk, who], send_sem.at[0], tab_sem.at[blk, who], up
        ).wait_recv()

    pl.semaphore_wait(barrier, jnp.where(end, 7, 6))
    sends = []

    def go(blk, who, target, cond=None):
        copy = table_copy(blk, who, len(sends), target)
        if cond is None:
            copy.start()
        else:
            pl.when(cond)(lambda: copy.start())
        sends.append((copy, cond))

    def halo(who):
        go(1, who, up, has_up)
        go(2, who, down, has_down)

    go(0, ch, other)
    go(end_out, ch, second_end, end)
    go(end_out, ch, first_end, end)
    for off in (2, 1, 3):
        go(0, ch, peer(off))
    halo(ch)

    for load in loads[1:6]:
        load.wait()

    spread = one_where(lax.rem(iota((16, EDGES), 1), 16) == iota((16, EDGES), 0))
    pick = (iota((8, EDGES), 1) // 16) == iota((8, EDGES), 0)

    def edge_row(ref):
        wide = dot(ref[...].astype(F32).astype(BF16), spread)
        return jnp.sum(jnp.where(pick, wide, 0.0), axis=0, keepdims=True)

    src = edge_row(src_ref)
    turns = edge_row(turn_ref)
    lane = iota((1, EDGES), 1)
    atom = lax.rem(lane, 16)
    ghost = jnp.zeros((1, EDGES), F32)
    count = jnp.zeros((1, EDGES), jnp.int32)
    for a in range(16):
        ghost = jnp.where(src == 16.0 + a, slot_ref[a].astype(F32), ghost)
        count = jnp.where(atom == a, cnt_ref[a], count)
    nowhere = -1000.0
    index = (
        jnp.where(src < 16.0, src, nowhere),
        jnp.where((src >= 16.0) & (src < 24.0), ghost, nowhere),
        jnp.where(src >= 24.0, ghost, nowhere),
    )
    row_id = iota((EDGES, EDGES), 0).astype(F32)
    lane_id = iota((EDGES, EDGES), 1).astype(F32)
    for blk in range(4):
        idx = atom.astype(F32) if blk == 3 else index[blk]
        wide = jnp.broadcast_to(idx, (EDGES, EDGES))
        tall = wide.T
        for c in range(8):
            forth = one_where(row_id == wide + 16.0 * c)
            fro = one_where(lane_id == tall + 16.0 * c)
            if blk == 3:
                gat_tile[:, c * 128 : c * 128 + 128] = forth
                sca_tile[c * 128 : c * 128 + 128, :] = fro
            else:
                gat[blk * 128 : blk * 128 + 128, c * 128 : c * 128 + 128] = forth
                sca[c * 128 : c * 128 + 128, blk * 128 : blk * 128 + 128] = fro

    chosen = one_where(iota((256, EDGES), 0).astype(F32) == jnp.broadcast_to(turns, (256, EDGES)))
    whole = wig_ref[...]
    first = whole.astype(BF16)
    rest = whole - first.astype(F32)
    second = rest.astype(BF16)
    third = (rest - second.astype(F32)).astype(BF16)
    wige[...] = dot(first, chosen) + (dot(second, chosen) + dot(third, chosen))

    for load in loads[6:]:
        load.wait()

    def keep_p(n, pos, value):
        ps[pos] = value

    rotate_in(dot(to_rows(g_ref, pad).astype(BF16), gat_tile[...]), wige, feats, keep_p)

    for lev in range(7):
        tile = w0_ref[:, lev].reshape(112, 128).astype(F32)
        wt0[lev * 128 : lev * 128 + 128, :] = (
            jnp.concatenate([tile, jnp.zeros((16, 128), F32)], 0).T.astype(BF16)
        )
    for ref, out, n in ((w1_ref, wt1, 6), (w2_ref, wt2, 5)):
        for part in range(2):
            for lev in range(n):
                tile = ref[part, :, lev].reshape(n * 16, 128).astype(F32)
                tile = jnp.concatenate([tile, jnp.zeros((128 - n * 16, 128), F32)], 0)
                out[lev * 128 : lev * 128 + 128, part * 128 : part * 128 + 128] = (
                    tile.T.astype(BF16)
                )
    back[...] = jnp.zeros_like(back)

    near = [zh * 4 + lax.rem(xi + off, 4) for off in (1, 3, 2)]
    far = [(1 - zh) * 4 + lax.rem(xi + off, 4) for off in (1, 3, 2)]
    arrival(0, near[0])
    halo(near[0])
    arrival(0, near[1])
    halo(near[1])
    arrival(0, near[2])
    halo(near[2])

    def end_copy(n, who, target):
        return rcopy(
            tab.at[end_in, who],
            tab.at[end_in, who],
            end_send.at[n],
            tab_sem.at[end_in, who],
            target,
        )

    @pl.when(end)
    def _():
        for n, who in enumerate((mirror, ch)):
            end_copy(0, who, first_end).wait_recv()
            for j, off in enumerate((2, 1, 3)):
                end_copy(n * 3 + j, who, peer(off)).start()

    arrival(0, mirror)
    for off in (2, 1, 3):
        go(0, mirror, peer(off))
    halo(mirror)
    for who in far:
        arrival(0, who)
        halo(who)

    def halo_arrival(blk, who):
        came = jnp.logical_and(end, jnp.logical_and(lax.rem(who, 4) == xi, blk == end_in))
        pl.when(jnp.logical_not(came))(lambda: arrival(blk, who))

    def pair_in(i, carry):
        side = lax.rem(zh + i // 2, 2)
        both = [side * 4 + lax.rem(xi + lax.rem(2 * i, 4) + n, 4) for n in range(2)]
        for who in both:
            halo_arrival(1, who)
            halo_arrival(2, who)
        lhs = jnp.concatenate(
            [jnp.concatenate([tab[0, who], tab[1, who], tab[2, who]], 1) for who in both], 0
        )

        def keep(n, pos, value):
            rot[pl.ds(pl.multiple_of(pos * 128 + both[n] * 16, 16), 16), :] = value.astype(BF16)

        rotate_in(dot(lhs, gat[...]), wige, feats, keep)
        return carry

    lax.fori_loop(0, 4, pair_in, 0)
    for copy, cond in sends:
        if cond is None:
            copy.wait_send()
        else:
            pl.when(cond)(lambda copy=copy: copy.wait_send())

    @pl.when(end)
    def _():
        for n, who in enumerate((mirror, ch)):
            for j, off in enumerate((2, 1, 3)):
                end_copy(n * 3 + j, who, peer(off)).wait_send()

    w0 = jnp.concatenate([w0_ref[:, lev].reshape(112, 128) for lev in range(7)], 1)
    y0 = dot(w0, rot[0:896, :])
    ys[0:7] = y0.reshape(7, 16, EDGES)
    for ref, n, start in ((w1_ref, 6, 7), (w2_ref, 5, 19)):
        lhs = jnp.concatenate(
            [ref[:, :, lev].reshape(2 * n * 16, 128) for lev in range(n)], 1
        )
        plus = rot[start * 128 : (start + n) * 128, :]
        minus = rot[(start + n) * 128 : (start + 2 * n) * 128, :]
        both = dot(lhs, jnp.concatenate([plus, minus], 1))
        half = n * 16
        ys[start : start + n] = (both[:half, :128] - both[half:, 128:]).reshape(n, 16, EDGES)
        ys[start + n : start + 2 * n] = (both[:half, 128:] + both[half:, :128]).reshape(
            n, 16, EDGES
        )

    attn = jnp.zeros((16, EDGES), F32)
    rows = iota((16, EDGES), 0)
    for t in range(16):
        attn = jnp.where(rows == t, attn_ref[t], attn)
    scalar = ys[0]
    gate = jax.nn.sigmoid(scalar)
    score = jnp.sum(scalar * gate * attn, axis=0, keepdims=True)
    live = jnp.broadcast_to((lane // 16) < count, (8, EDGES))
    score = jnp.broadcast_to(score, (8, EDGES))
    masked = jnp.where(live, score, -1e30)
    top = over_slots(masked, jnp.maximum)
    weight = jnp.exp(jnp.where(live, score - top, -1e30))
    weight = weight / over_slots(weight, jnp.add)
    weight2 = jnp.concatenate([weight, weight], 0)
    inner = ys[0] * ps[0]
    for pos in range(1, 29):
        inner = inner + ys[pos] * ps[pos]
    dweight = jnp.broadcast_to(jnp.sum(inner * gate, axis=0, keepdims=True), (8, EDGES))
    mean = over_slots(weight * dweight, jnp.add)
    dscore = weight * (dweight - mean)
    dscore2 = jnp.concatenate([dscore, dscore], 0)
    slope = gate * (1.0 - gate)
    dscalar = weight2 * inner * slope + dscore2 * attn * (gate + scalar * slope)
    factor = weight2 * gate

    nil = jnp.zeros((16, EDGES), F32)
    dys = [ps[pos] * factor for pos in range(29)]
    dys[0] = dys[0] + dscalar
    dy0 = jnp.concatenate(dys[0:7] + [nil], 0).astype(BF16)
    drot[0:896, :] = dot(wt0[...], dy0).astype(BF16)
    for out, n, start in ((wt1, 6, 7), (wt2, 5, 19)):
        plus = jnp.concatenate(dys[start : start + n] + [nil] * (8 - n), 0).astype(BF16)
        minus = jnp.concatenate(dys[start + n : start + 2 * n] + [nil] * (8 - n), 0).astype(BF16)
        rhs = jnp.concatenate(
            [jnp.concatenate([plus, minus], 1), jnp.concatenate([minus, -plus], 1)], 0
        )
        both = dot(out[...], rhs)
        drot[start * 128 : (start + n) * 128, :] = both[:, :128].astype(BF16)
        drot[(start + n) * 128 : (start + 2 * n) * 128, :] = both[:, 128:].astype(BF16)

    def group_of(i):
        half = i // 4
        j = lax.rem(i, 4)
        off = jnp.where(j == 0, 2, jnp.where(j == 1, 1, jnp.where(j == 2, 3, 0)))
        return lax.rem(1 - zh + half, 2) * 4 + lax.rem(xi + off, 4)

    def to_down(who):
        return rcopy(
            ghost_out.at[0, who],
            from_above.at[who],
            ghost_send.at[0, who],
            ghost_recv.at[0, who],
            down,
        )

    def to_up(who):
        return rcopy(
            ghost_out.at[1, who],
            from_below.at[who],
            ghost_send.at[1, who],
            ghost_recv.at[1, who],
            up,
        )

    def pair_out(i, carry):
        both = [group_of(2 * i + n) for n in range(2)]

        def read(n, pos):
            start = pl.multiple_of(pos * 128 + both[n] * 16, 16)
            value = drot[pl.ds(start, 16), :].astype(F32)
            return value[0:8], value[8:16]

        rotate_out(read, wige, back, 2)
        out = dot(across(back, 2).astype(BF16), sca[...])
        for n, who in enumerate(both):
            part = out[n * ROWS : (n + 1) * ROWS]
            ghost_out[0, who] = part[:, 128:256].astype(BF16)
            ghost_out[1, who] = part[:, 256:384].astype(BF16)
            pl.when(has_down)(lambda who=who: to_down(who).start())
            pl.when(has_up)(lambda who=who: to_up(who).start())
            accum[who] = part[:, 0:128]
        return carry

    @pl.when(d == doms - 1)
    def _():
        from_above[...] = jnp.zeros_like(from_above)

    @pl.when(d == 0)
    def _():
        from_below[...] = jnp.zeros_like(from_below)

    lax.fori_loop(0, 4, pair_out, 0)

    offs = (2, 1, 3)

    def end_peer(i):
        half = i // 3
        off = offs[i % 3]
        who = ((zh + 1 - half) % 2) * 4 + lax.rem(xi + off, 4)
        return rcopy(
            ghost_out.at[end_side, who], end_x.at[i], end_send.at[i], end_recv.at[i], peer(off)
        )

    def end_home(half):
        target = (second_end, first_end)[half]
        return rcopy(
            end_sum.at[half], end_got.at[half], end_last.at[half], end_last.at[2 + half], target
        )

    @pl.when(end)
    def _():
        for i in range(6):
            end_peer(i).start()

    def to_peer(i, off):
        return rcopy(x_out.at[i], x_in.at[i], xs_send.at[i], xs_recv.at[i], peer(off))

    def finish(i):
        who = group_of(i)
        pl.when(has_up)(lambda: to_down(who).wait_recv())
        pl.when(has_down)(lambda: to_up(who).wait_recv())
        return accum[who] + from_above[who].astype(F32) + from_below[who].astype(F32)

    for half in range(2):
        for j in range(3):
            x_out[half * 3 + j] = finish(half * 4 + j).astype(BF16)
            to_peer(half * 3 + j, offs[j]).start()
        red[half] = finish(half * 4 + 3)

    def gathered(half):
        total = red[half]
        for j in range(3):
            to_peer(half * 3 + j, offs[j]).wait_recv()
            total = total + x_in[half * 3 + j].astype(F32)
        return total

    @pl.when(end)
    def _():
        for half in range(2):
            who = ((zh + 1 - half) % 2) * 4 + xi
            total = ghost_out[end_side, who].astype(F32)
            for j in range(3):
                end_peer(half * 3 + j).wait_recv()
                total = total + end_x[half * 3 + j].astype(F32)
            end_sum[half] = total.astype(BF16)
            end_home(half).start()

    z_out[...] = gathered(0).astype(BF16)
    across_z = rcopy(z_out, z_in, zs_send.at[0], zs_recv.at[0], other)
    across_z.start()

    def read_z(n, pos):
        value = ys[pos] * factor
        return value[0:8], value[8:16]

    rotate_out(read_z, wige, back, 1)
    wide = across(back, 1)
    first = wide.astype(BF16)
    second = (wide - first.astype(F32)).astype(BF16)
    agg = dot(first, sca_tile[...]) + dot(second, sca_tile[...])
    upd_ref[...] = from_rows(agg)

    red[1] = gathered(1)

    @pl.when(end)
    def _():
        end_home(0).wait_recv()
        end_home(1).wait_recv()
        red[1] = red[1] + (end_got[0].astype(F32) + end_got[1].astype(F32))

    for i in range(6):
        to_peer(i, offs[i % 3]).wait_send()
    for i in range(8):
        pl.when(has_down)(lambda i=i: to_down(i).wait_send())
        pl.when(has_up)(lambda i=i: to_up(i).wait_send())

    @pl.when(end)
    def _():
        for i in range(6):
            end_peer(i).wait_send()
        end_home(0).wait_send()
        end_home(1).wait_send()
    across_z.wait_send()
    across_z.wait_recv()
    grad = red[1] + z_in[...].astype(F32)
    grad_ref[...] = from_rows(grad)


def on_device(
    node_irreps,
    out_grad,
    edge_source,
    edge_rotation,
    edge_count,
    ghost_slot,
    wigner,
    so2_m0,
    so2_m1,
    so2_m2,
    attn_vector,
):
    vmem = pl.BlockSpec(memory_space=pltpu.VMEM)
    hbm = pl.BlockSpec(memory_space=pltpu.HBM)
    block = (ROWS, 128)
    dma = pltpu.SemaphoreType.DMA
    upd, grad = pl.pallas_call(
        body,
        out_shape=(
            jax.ShapeDtypeStruct((16, 16, K), F32),
            jax.ShapeDtypeStruct((16, 16, K), F32),
        ),
        in_specs=[hbm] * 11,
        out_specs=(vmem, vmem),
        scratch_shapes=[
            pltpu.VMEM((16, 16, K), BF16),
            pltpu.VMEM((16, 16, K), BF16),
            pltpu.VMEM((8, 16), jnp.int32),
            pltpu.VMEM((8, 16), jnp.int32),
            pltpu.SMEM((16,), jnp.int32),
            pltpu.SMEM((16,), jnp.int32),
            pltpu.VMEM((455, 256), F32),
            pltpu.VMEM((7, 7, 16, 128), BF16),
            pltpu.VMEM((2, 6, 6, 16, 128), BF16),
            pltpu.VMEM((2, 5, 5, 16, 128), BF16),
            pltpu.SMEM((16,), F32),
            dma((11,)),
            pltpu.VMEM((3, 8) + block, BF16),
            pltpu.VMEM((256, 128), F32),
            pltpu.VMEM((455, EDGES), F32),
            pltpu.VMEM((384, 1024), BF16),
            pltpu.VMEM((1024, 384), BF16),
            pltpu.VMEM((128, 1024), BF16),
            pltpu.VMEM((1024, 128), BF16),
            pltpu.VMEM((2, 8 * PITCH, 128), F32),
            pltpu.VMEM((2, 8 * PITCH, 128), F32),
            pltpu.VMEM((29 * 128, EDGES), BF16),
            pltpu.VMEM((29 * 128, EDGES), BF16),
            pltpu.VMEM((29, 16, EDGES), F32),
            pltpu.VMEM((29, 16, EDGES), F32),
            pltpu.VMEM((896, 128), BF16),
            pltpu.VMEM((768, 256), BF16),
            pltpu.VMEM((640, 256), BF16),
            pltpu.VMEM((8,) + block, F32),
            pltpu.VMEM((2, 8) + block, BF16),
            pltpu.VMEM((8,) + block, BF16),
            pltpu.VMEM((8,) + block, BF16),
            pltpu.VMEM((6,) + block, BF16),
            pltpu.VMEM((6,) + block, BF16),
            pltpu.VMEM(block, BF16),
            pltpu.VMEM(block, BF16),
            pltpu.VMEM((2,) + block, F32),
            pltpu.VMEM((6,) + block, BF16),
            pltpu.VMEM((2,) + block, BF16),
            pltpu.VMEM((2,) + block, BF16),
            dma((27,)),
            dma((3, 8)),
            dma((2, 8)),
            dma((2, 8)),
            dma((6,)),
            dma((6,)),
            dma((1,)),
            dma((1,)),
            dma((6,)),
            dma((6,)),
            dma((4,)),
        ],
        compiler_params=pltpu.CompilerParams(
            collective_id=0, has_side_effects=True, vmem_limit_bytes=24 * 1024 * 1024
        ),
        name="layer",
    )(
        *(
            pltpu.with_memory_space_constraint(array, pltpu.HBM)
            for array in (
                jnp.transpose(node_irreps, (1, 2, 0)),
                jnp.transpose(out_grad, (1, 2, 0)),
                edge_source,
                edge_rotation,
                edge_count,
                ghost_slot,
                wigner,
                jnp.transpose(so2_m0, (0, 2, 1, 3)),
                jnp.transpose(so2_m1, (0, 1, 3, 2, 4)),
                jnp.transpose(so2_m2, (0, 1, 3, 2, 4)),
                attn_vector,
            )
        )
    )
    updated = node_irreps.astype(F32) + jnp.transpose(upd, (2, 0, 1))
    irreps_grad = out_grad.astype(F32) + jnp.transpose(grad, (2, 0, 1))
    return updated.astype(BF16), irreps_grad


def solution(mesh):
    placed = (
        P(None, "ch", "dom"),
        P(None, "ch", "dom"),
        P(None, "dom"),
        P(None, "dom"),
        P("dom"),
        P("dom"),
        P(None, "dom"),
        P(None, "ch", None, None),
        P(None, None, "ch", None, None),
        P(None, None, "ch", None, None),
        P("ch"),
    )
    return jax.shard_map(
        on_device,
        mesh=mesh,
        in_specs=placed,
        out_specs=(P(None, "ch", "dom"), P(None, "ch", "dom")),
        check_vma=False,
    )
```

```python
import jax
import jax.numpy as jnp
from jax import lax
from jax.experimental import pallas as pl
from jax.experimental.pallas import tpu as pltpu
from jax.sharding import PartitionSpec as P

LMAX = 6
MMAX = 2
K = 49
OWN = 16
EDGES = 128
KP = 56
ROWS = 2 * KP
PITCH = 116
F32 = jnp.float32
BF16 = jnp.bfloat16
MESH = pl.DeviceIdType.MESH


def rows_of_levels():
    levels = []
    offset = 0
    for level in range(LMAX + 1):
        width = 2 * level + 1
        reach = min(level, MMAX)
        orders = list(range(-reach, reach + 1))
        levels.append((level, width, offset, orders))
        offset += width * width
    return levels


LEVELS = rows_of_levels()


def place(level, order):
    if order == 0:
        return level
    if order == 1:
        return 6 + level
    if order == -1:
        return 12 + level
    if order == 2:
        return 17 + level
    return 22 + level


def iota(shape, dim):
    return lax.broadcasted_iota(jnp.int32, shape, dim)


def one_where(cond):
    return jnp.where(cond, 1.0, 0.0).astype(BF16)


def spin(x, shift):
    return pltpu.roll(x, shift, 1)


def over_slots(x, join):
    parts = [x] + [spin(x, shift) for shift in range(OWN, EDGES, OWN)]
    while len(parts) > 1:
        parts = [join(parts[i], parts[i + 1]) for i in range(0, len(parts), 2)]
    return parts[0]


def dot(a, b):
    return jnp.dot(a, b, preferred_element_type=F32)


def turn(wige, level, width, offset, order, col):
    row = offset + (level + order) * width + col
    return jnp.broadcast_to(wige[row : row + 1, :], (8, EDGES))


def rotate_in(mixed, wige, feats, write):
    groups = range(mixed.shape[0] // ROWS)
    for n in groups:
        for c in range(8):
            feats[n, c * PITCH : c * PITCH + ROWS, :] = mixed[
                n * ROWS : (n + 1) * ROWS, c * EDGES : (c + 1) * EDGES
            ]
    for level, width, offset, orders in LEVELS:
        acc = {}
        for col in range(width):
            k = level * level + col
            parts = [
                feats[n, pl.ds(start + k, 8, stride=PITCH), :] for n in groups for start in (0, KP)
            ]
            for order in orders:
                w = turn(wige, level, width, offset, order, col)
                if col == 0:
                    acc[order] = [w * part for part in parts]
                else:
                    acc[order] = [old + w * part for old, part in zip(acc[order], parts)]
        for order in orders:
            for n in groups:
                write(n, place(level, order), jnp.concatenate(acc[order][2 * n : 2 * n + 2], 0))


def rotate_out(read, wige, back, count):
    for level, width, offset, orders in LEVELS:
        mine = {
            order: [part for n in range(count) for part in read(n, place(level, order))]
            for order in orders
        }
        for col in range(width):
            k = level * level + col
            total = None
            for order in orders:
                w = turn(wige, level, width, offset, order, col)
                if total is None:
                    total = [w * part for part in mine[order]]
                else:
                    total = [old + w * part for old, part in zip(total, mine[order])]
            for n in range(count):
                back[n, pl.ds(k, 8, stride=PITCH), :] = total[2 * n]
                back[n, pl.ds(KP + k, 8, stride=PITCH), :] = total[2 * n + 1]


def across(back, count):
    return jnp.concatenate(
        [
            jnp.concatenate([back[n, c * PITCH : c * PITCH + ROWS, :] for c in range(8)], 1)
            for n in range(count)
        ],
        0,
    )


def to_rows(ref, pad):
    pad[...] = jnp.zeros_like(pad)
    pad[:, 0:K] = ref[...].astype(F32).reshape(256, K)
    low = pad[0:128, :].T
    high = pad[128:256, :].T
    return jnp.concatenate([low[0:KP], high[0:KP]], 0)


def from_rows(rows):
    fill = jnp.zeros((128 - KP, 128), F32)
    low = jnp.concatenate([rows[0:KP], fill], 0).T
    high = jnp.concatenate([rows[KP:ROWS], fill], 0).T
    return jnp.concatenate([low, high], 0)[:, 0:K].reshape(16, 16, K)


def body(
    x_hbm,
    g_hbm,
    src_hbm,
    turn_hbm,
    cnt_hbm,
    slot_hbm,
    wig_hbm,
    w0_hbm,
    w1_hbm,
    w2_hbm,
    attn_hbm,
    upd_ref,
    grad_ref,
    x_ref,
    g_ref,
    src_ref,
    turn_ref,
    cnt_ref,
    slot_ref,
    wig_ref,
    w0_ref,
    w1_ref,
    w2_ref,
    attn_ref,
    load_sem,
    tab,
    pad,
    wige,
    gat,
    sca,
    gat_tile,
    sca_tile,
    feats,
    back,
    rot,
    drot,
    ys,
    ps,
    wt0,
    wt1,
    wt2,
    accum,
    ghost_out,
    from_above,
    from_below,
    x_out,
    x_in,
    z_out,
    z_in,
    red,
    end_x,
    end_sum,
    end_got,
    send_sem,
    tab_sem,
    ghost_send,
    ghost_recv,
    xs_send,
    xs_recv,
    zs_send,
    zs_recv,
    end_send,
    end_recv,
    end_last,
):
    doms = lax.axis_size("dom")
    d = lax.axis_index("dom")
    ch = lax.axis_index("ch")
    zh = ch // 4
    xi = lax.rem(ch, 4)
    mirror = lax.rem(ch + 4, 8)
    up = (lax.rem(d + 1, doms), ch)
    down = (lax.rem(d + doms - 1, doms), ch)
    other = (d, mirror)

    def peer(off):
        return (d, zh * 4 + lax.rem(xi + off, 4))

    has_up = d != doms - 1
    has_down = d != 0
    end = jnp.logical_or(d == 0, d == doms - 1)
    first_end = (doms - 1 - d, ch)
    second_end = (doms - 1 - d, mirror)
    end_in = jnp.where(d == 0, 1, 2)
    end_out = jnp.where(d == 0, 2, 1)
    end_side = jnp.where(d == 0, 0, 1)

    barrier = pltpu.get_barrier_semaphore()

    def greet(target):
        pl.semaphore_signal(barrier, inc=1, device_id=target, device_id_type=MESH)

    for target in (other, peer(1), peer(2), peer(3)):
        greet(target)
    pl.when(has_up)(lambda: greet(up))
    pl.when(has_down)(lambda: greet(down))

    @pl.when(end)
    def _():
        greet(first_end)
        greet(second_end)

    loads = [
        pltpu.make_async_copy(src, dst, load_sem.at[n])
        for n, (src, dst) in enumerate(
            (
                (x_hbm, x_ref),
                (src_hbm, src_ref),
                (turn_hbm, turn_ref),
                (cnt_hbm, cnt_ref),
                (slot_hbm, slot_ref),
                (wig_hbm, wig_ref),
                (g_hbm, g_ref),
                (w0_hbm, w0_ref),
                (w1_hbm, w1_ref),
                (w2_hbm, w2_ref),
                (attn_hbm, attn_ref),
            )
        )
    ]
    for load in loads:
        load.start()
    loads[0].wait()
    tab[0, ch] = to_rows(x_ref, pad).astype(BF16)

    def rcopy(src, dst, ssem, rsem, target):
        return pltpu.make_async_remote_copy(
            src_ref=src,
            dst_ref=dst,
            send_sem=ssem,
            recv_sem=rsem,
            device_id=target,
            device_id_type=MESH,
        )

    def table_copy(blk, who, n, target):
        return rcopy(
            tab.at[0, who], tab.at[blk, who], send_sem.at[n], tab_sem.at[blk, who], target
        )

    def arrival(blk, who):
        return rcopy(
            tab.at[0, who], tab.at[blk, who], send_sem.at[0], tab_sem.at[blk, who], up
        ).wait_recv()

    pl.semaphore_wait(barrier, jnp.where(end, 7, 6))
    sends = []

    def go(blk, who, target, cond=None):
        copy = table_copy(blk, who, len(sends), target)
        if cond is None:
            copy.start()
        else:
            pl.when(cond)(lambda: copy.start())
        sends.append((copy, cond))

    def halo(who):
        go(1, who, up, has_up)
        go(2, who, down, has_down)

    go(0, ch, other)
    go(end_out, ch, second_end, end)
    go(end_out, ch, first_end, end)
    for off in (2, 1, 3):
        go(0, ch, peer(off))
    halo(ch)

    for load in loads[1:6]:
        load.wait()

    spread = one_where(lax.rem(iota((16, EDGES), 1), 16) == iota((16, EDGES), 0))
    pick = (iota((8, EDGES), 1) // 16) == iota((8, EDGES), 0)

    def edge_row(ref):
        wide = dot(ref[...].astype(F32).astype(BF16), spread)
        return jnp.sum(jnp.where(pick, wide, 0.0), axis=0, keepdims=True)

    src = edge_row(src_ref)
    turns = edge_row(turn_ref)
    lane = iota((1, EDGES), 1)
    atom = lax.rem(lane, 16)
    ghost = jnp.zeros((1, EDGES), F32)
    count = jnp.zeros((1, EDGES), jnp.int32)
    for a in range(16):
        ghost = jnp.where(src == 16.0 + a, slot_ref[a].astype(F32), ghost)
        count = jnp.where(atom == a, cnt_ref[a], count)
    nowhere = -1000.0
    index = (
        jnp.where(src < 16.0, src, nowhere),
        jnp.where((src >= 16.0) & (src < 24.0), ghost, nowhere),
        jnp.where(src >= 24.0, ghost, nowhere),
    )
    row_id = iota((EDGES, EDGES), 0).astype(F32)
    lane_id = iota((EDGES, EDGES), 1).astype(F32)
    for blk in range(4):
        idx = atom.astype(F32) if blk == 3 else index[blk]
        wide = jnp.broadcast_to(idx, (EDGES, EDGES))
        tall = wide.T
        for c in range(8):
            forth = one_where(row_id == wide + 16.0 * c)
            fro = one_where(lane_id == tall + 16.0 * c)
            if blk == 3:
                gat_tile[:, c * 128 : c * 128 + 128] = forth
                sca_tile[c * 128 : c * 128 + 128, :] = fro
            else:
                gat[blk * 128 : blk * 128 + 128, c * 128 : c * 128 + 128] = forth
                sca[c * 128 : c * 128 + 128, blk * 128 : blk * 128 + 128] = fro

    chosen = one_where(iota((256, EDGES), 0).astype(F32) == jnp.broadcast_to(turns, (256, EDGES)))
    whole = wig_ref[...]
    first = whole.astype(BF16)
    rest = whole - first.astype(F32)
    second = rest.astype(BF16)
    third = (rest - second.astype(F32)).astype(BF16)
    wige[...] = dot(first, chosen) + (dot(second, chosen) + dot(third, chosen))

    for load in loads[6:]:
        load.wait()

    def keep_p(n, pos, value):
        ps[pos] = value

    rotate_in(dot(to_rows(g_ref, pad).astype(BF16), gat_tile[...]), wige, feats, keep_p)

    for lev in range(7):
        tile = w0_ref[:, lev].reshape(112, 128).astype(F32)
        wt0[lev * 128 : lev * 128 + 128, :] = (
            jnp.concatenate([tile, jnp.zeros((16, 128), F32)], 0).T.astype(BF16)
        )
    for ref, out, n in ((w1_ref, wt1, 6), (w2_ref, wt2, 5)):
        for part in range(2):
            for lev in range(n):
                tile = ref[part, :, lev].reshape(n * 16, 128).astype(F32)
                tile = jnp.concatenate([tile, jnp.zeros((128 - n * 16, 128), F32)], 0)
                out[lev * 128 : lev * 128 + 128, part * 128 : part * 128 + 128] = (
                    tile.T.astype(BF16)
                )
    back[...] = jnp.zeros_like(back)

    near = [zh * 4 + lax.rem(xi + off, 4) for off in (1, 3, 2)]
    far = [(1 - zh) * 4 + lax.rem(xi + off, 4) for off in (1, 3, 2)]
    arrival(0, near[0])
    halo(near[0])
    arrival(0, near[1])
    halo(near[1])
    arrival(0, near[2])
    halo(near[2])

    def end_copy(n, who, target):
        return rcopy(
            tab.at[end_in, who],
            tab.at[end_in, who],
            end_send.at[n],
            tab_sem.at[end_in, who],
            target,
        )

    @pl.when(end)
    def _():
        for n, who in enumerate((mirror, ch)):
            end_copy(0, who, first_end).wait_recv()
            for j, off in enumerate((2, 1, 3)):
                end_copy(n * 3 + j, who, peer(off)).start()

    arrival(0, mirror)
    for off in (2, 1, 3):
        go(0, mirror, peer(off))
    halo(mirror)
    for who in far:
        arrival(0, who)
        halo(who)

    def halo_arrival(blk, who):
        came = jnp.logical_and(end, jnp.logical_and(lax.rem(who, 4) == xi, blk == end_in))
        pl.when(jnp.logical_not(came))(lambda: arrival(blk, who))

    def pair_in(i, carry):
        side = lax.rem(zh + i // 2, 2)
        both = [side * 4 + lax.rem(xi + lax.rem(2 * i, 4) + n, 4) for n in range(2)]
        for who in both:
            halo_arrival(1, who)
            halo_arrival(2, who)
        lhs = jnp.concatenate(
            [jnp.concatenate([tab[0, who], tab[1, who], tab[2, who]], 1) for who in both], 0
        )

        def keep(n, pos, value):
            rot[pl.ds(pl.multiple_of(pos * 128 + both[n] * 16, 16), 16), :] = value.astype(BF16)

        rotate_in(dot(lhs, gat[...]), wige, feats, keep)
        return carry

    lax.fori_loop(0, 4, pair_in, 0)
    for copy, cond in sends:
        if cond is None:
            copy.wait_send()
        else:
            pl.when(cond)(lambda copy=copy: copy.wait_send())

    @pl.when(end)
    def _():
        for n, who in enumerate((mirror, ch)):
            for j, off in enumerate((2, 1, 3)):
                end_copy(n * 3 + j, who, peer(off)).wait_send()

    w0 = jnp.concatenate([w0_ref[:, lev].reshape(112, 128) for lev in range(7)], 1)
    y0 = dot(w0, rot[0:896, :])
    ys[0:7] = y0.reshape(7, 16, EDGES)
    for ref, n, start in ((w1_ref, 6, 7), (w2_ref, 5, 19)):
        lhs = jnp.concatenate(
            [ref[:, :, lev].reshape(2 * n * 16, 128) for lev in range(n)], 1
        )
        plus = rot[start * 128 : (start + n) * 128, :]
        minus = rot[(start + n) * 128 : (start + 2 * n) * 128, :]
        both = dot(lhs, jnp.concatenate([plus, minus], 1))
        half = n * 16
        ys[start : start + n] = (both[:half, :128] - both[half:, 128:]).reshape(n, 16, EDGES)
        ys[start + n : start + 2 * n] = (both[:half, 128:] + both[half:, :128]).reshape(
            n, 16, EDGES
        )

    attn = jnp.zeros((16, EDGES), F32)
    rows = iota((16, EDGES), 0)
    for t in range(16):
        attn = jnp.where(rows == t, attn_ref[t], attn)
    scalar = ys[0]
    gate = jax.nn.sigmoid(scalar)
    score = jnp.sum(scalar * gate * attn, axis=0, keepdims=True)
    live = jnp.broadcast_to((lane // 16) < count, (8, EDGES))
    score = jnp.broadcast_to(score, (8, EDGES))
    masked = jnp.where(live, score, -1e30)
    top = over_slots(masked, jnp.maximum)
    weight = jnp.exp(jnp.where(live, score - top, -1e30))
    weight = weight / over_slots(weight, jnp.add)
    weight2 = jnp.concatenate([weight, weight], 0)
    inner = ys[0] * ps[0]
    for pos in range(1, 29):
        inner = inner + ys[pos] * ps[pos]
    dweight = jnp.broadcast_to(jnp.sum(inner * gate, axis=0, keepdims=True), (8, EDGES))
    mean = over_slots(weight * dweight, jnp.add)
    dscore = weight * (dweight - mean)
    dscore2 = jnp.concatenate([dscore, dscore], 0)
    slope = gate * (1.0 - gate)
    dscalar = weight2 * inner * slope + dscore2 * attn * (gate + scalar * slope)
    factor = weight2 * gate

    nil = jnp.zeros((16, EDGES), F32)
    gated = [ps[pos] * gate for pos in range(29)]
    for out, n, start in ((wt1, 6, 7), (wt2, 5, 19)):
        plus = jnp.concatenate(gated[start : start + n] + [nil] * (8 - n), 0).astype(BF16)
        minus = jnp.concatenate(gated[start + n : start + 2 * n] + [nil] * (8 - n), 0).astype(BF16)
        rhs = jnp.concatenate(
            [jnp.concatenate([plus, minus], 1), jnp.concatenate([minus, -plus], 1)], 0
        )
        both = dot(out[...], rhs)
        tall = jnp.broadcast_to(weight[0:1], (n * 128, EDGES))
        drot[start * 128 : (start + n) * 128, :] = (both[:, :128] * tall).astype(BF16)
        drot[(start + n) * 128 : (start + 2 * n) * 128, :] = (both[:, 128:] * tall).astype(BF16)
    dys = [gated[pos] * weight2 for pos in range(7)]
    dys[0] = dys[0] + dscalar
    dy0 = jnp.concatenate(dys + [nil], 0).astype(BF16)
    drot[0:896, :] = dot(wt0[...], dy0).astype(BF16)

    def group_of(i):
        half = i // 4
        j = lax.rem(i, 4)
        off = jnp.where(j == 0, 2, jnp.where(j == 1, 1, jnp.where(j == 2, 3, 0)))
        return lax.rem(1 - zh + half, 2) * 4 + lax.rem(xi + off, 4)

    def to_down(who):
        return rcopy(
            ghost_out.at[0, who],
            from_above.at[who],
            ghost_send.at[0, who],
            ghost_recv.at[0, who],
            down,
        )

    def to_up(who):
        return rcopy(
            ghost_out.at[1, who],
            from_below.at[who],
            ghost_send.at[1, who],
            ghost_recv.at[1, who],
            up,
        )

    offs = (2, 1, 3)

    def end_part(i, who, target):
        return rcopy(
            ghost_out.at[end_side, who], end_x.at[i], end_send.at[i], end_recv.at[i], target
        )

    def end_peer(i):
        half = i // 3
        off = offs[i % 3]
        who = ((zh + 1 - half) % 2) * 4 + lax.rem(xi + off, 4)
        return end_part(i, who, peer(off))

    def pair_out(i, carry):
        both = [group_of(2 * i + n) for n in range(2)]

        def read(n, pos):
            start = pl.multiple_of(pos * 128 + both[n] * 16, 16)
            value = drot[pl.ds(start, 16), :].astype(F32)
            return value[0:8], value[8:16]

        rotate_out(read, wige, back, 2)
        out = dot(across(back, 2).astype(BF16), sca[...])
        for n, who in enumerate(both):
            part = out[n * ROWS : (n + 1) * ROWS]
            ghost_out[0, who] = part[:, 128:256].astype(BF16)
            ghost_out[1, who] = part[:, 256:384].astype(BF16)
            pl.when(has_down)(lambda who=who: to_down(who).start())
            pl.when(has_up)(lambda who=who: to_up(who).start())
            accum[who] = part[:, 0:128]

        odd = lax.rem(i, 2)

        @pl.when(end)
        def _():
            end_part((i // 2) * 3 + odd * 2, both[0], peer(2 + odd)).start()

        @pl.when(jnp.logical_and(end, odd == 0))
        def _():
            end_part((i // 2) * 3 + 1, both[1], peer(1)).start()

        return carry

    @pl.when(d == doms - 1)
    def _():
        from_above[...] = jnp.zeros_like(from_above)

    @pl.when(d == 0)
    def _():
        from_below[...] = jnp.zeros_like(from_below)

    lax.fori_loop(0, 4, pair_out, 0)

    def end_home(half):
        target = (second_end, first_end)[half]
        return rcopy(
            end_sum.at[half], end_got.at[half], end_last.at[half], end_last.at[2 + half], target
        )


    def to_peer(i, off):
        return rcopy(x_out.at[i], x_in.at[i], xs_send.at[i], xs_recv.at[i], peer(off))

    def finish(i):
        who = group_of(i)
        pl.when(has_up)(lambda: to_down(who).wait_recv())
        pl.when(has_down)(lambda: to_up(who).wait_recv())
        return accum[who] + from_above[who].astype(F32) + from_below[who].astype(F32)

    for half in range(2):
        for j in range(3):
            x_out[half * 3 + j] = finish(half * 4 + j).astype(BF16)
            to_peer(half * 3 + j, offs[j]).start()
        red[half] = finish(half * 4 + 3)

    def gathered(half):
        total = red[half]
        for j in range(3):
            to_peer(half * 3 + j, offs[j]).wait_recv()
            total = total + x_in[half * 3 + j].astype(F32)
        return total

    @pl.when(end)
    def _():
        for half in range(2):
            who = ((zh + 1 - half) % 2) * 4 + xi
            total = ghost_out[end_side, who].astype(F32)
            for j in range(3):
                end_peer(half * 3 + j).wait_recv()
                total = total + end_x[half * 3 + j].astype(F32)
            end_sum[half] = total.astype(BF16)
            end_home(half).start()

    z_out[...] = gathered(0).astype(BF16)
    across_z = rcopy(z_out, z_in, zs_send.at[0], zs_recv.at[0], other)
    across_z.start()

    def read_z(n, pos):
        value = ys[pos] * factor
        return value[0:8], value[8:16]

    rotate_out(read_z, wige, back, 1)
    wide = across(back, 1)
    first = wide.astype(BF16)
    second = (wide - first.astype(F32)).astype(BF16)
    agg = dot(first, sca_tile[...]) + dot(second, sca_tile[...])
    upd_ref[...] = from_rows(agg)

    red[1] = gathered(1)

    @pl.when(end)
    def _():
        end_home(0).wait_recv()
        end_home(1).wait_recv()
        red[1] = red[1] + (end_got[0].astype(F32) + end_got[1].astype(F32))

    for i in range(6):
        to_peer(i, offs[i % 3]).wait_send()
    for i in range(8):
        pl.when(has_down)(lambda i=i: to_down(i).wait_send())
        pl.when(has_up)(lambda i=i: to_up(i).wait_send())

    @pl.when(end)
    def _():
        for i in range(6):
            end_peer(i).wait_send()
        end_home(0).wait_send()
        end_home(1).wait_send()
    across_z.wait_send()
    across_z.wait_recv()
    grad = red[1] + z_in[...].astype(F32)
    grad_ref[...] = from_rows(grad)


def on_device(
    node_irreps,
    out_grad,
    edge_source,
    edge_rotation,
    edge_count,
    ghost_slot,
    wigner,
    so2_m0,
    so2_m1,
    so2_m2,
    attn_vector,
):
    vmem = pl.BlockSpec(memory_space=pltpu.VMEM)
    hbm = pl.BlockSpec(memory_space=pltpu.HBM)
    block = (ROWS, 128)
    dma = pltpu.SemaphoreType.DMA
    upd, grad = pl.pallas_call(
        body,
        out_shape=(
            jax.ShapeDtypeStruct((16, 16, K), F32),
            jax.ShapeDtypeStruct((16, 16, K), F32),
        ),
        in_specs=[hbm] * 11,
        out_specs=(vmem, vmem),
        scratch_shapes=[
            pltpu.VMEM((16, 16, K), BF16),
            pltpu.VMEM((16, 16, K), BF16),
            pltpu.VMEM((8, 16), jnp.int32),
            pltpu.VMEM((8, 16), jnp.int32),
            pltpu.SMEM((16,), jnp.int32),
            pltpu.SMEM((16,), jnp.int32),
            pltpu.VMEM((455, 256), F32),
            pltpu.VMEM((7, 7, 16, 128), BF16),
            pltpu.VMEM((2, 6, 6, 16, 128), BF16),
            pltpu.VMEM((2, 5, 5, 16, 128), BF16),
            pltpu.SMEM((16,), F32),
            dma((11,)),
            pltpu.VMEM((3, 8) + block, BF16),
            pltpu.VMEM((256, 128), F32),
            pltpu.VMEM((455, EDGES), F32),
            pltpu.VMEM((384, 1024), BF16),
            pltpu.VMEM((1024, 384), BF16),
            pltpu.VMEM((128, 1024), BF16),
            pltpu.VMEM((1024, 128), BF16),
            pltpu.VMEM((2, 8 * PITCH, 128), F32),
            pltpu.VMEM((2, 8 * PITCH, 128), F32),
            pltpu.VMEM((29 * 128, EDGES), BF16),
            pltpu.VMEM((29 * 128, EDGES), BF16),
            pltpu.VMEM((29, 16, EDGES), F32),
            pltpu.VMEM((29, 16, EDGES), F32),
            pltpu.VMEM((896, 128), BF16),
            pltpu.VMEM((768, 256), BF16),
            pltpu.VMEM((640, 256), BF16),
            pltpu.VMEM((8,) + block, F32),
            pltpu.VMEM((2, 8) + block, BF16),
            pltpu.VMEM((8,) + block, BF16),
            pltpu.VMEM((8,) + block, BF16),
            pltpu.VMEM((6,) + block, BF16),
            pltpu.VMEM((6,) + block, BF16),
            pltpu.VMEM(block, BF16),
            pltpu.VMEM(block, BF16),
            pltpu.VMEM((2,) + block, F32),
            pltpu.VMEM((6,) + block, BF16),
            pltpu.VMEM((2,) + block, BF16),
            pltpu.VMEM((2,) + block, BF16),
            dma((27,)),
            dma((3, 8)),
            dma((2, 8)),
            dma((2, 8)),
            dma((6,)),
            dma((6,)),
            dma((1,)),
            dma((1,)),
            dma((6,)),
            dma((6,)),
            dma((4,)),
        ],
        compiler_params=pltpu.CompilerParams(
            collective_id=0, has_side_effects=True, vmem_limit_bytes=24 * 1024 * 1024
        ),
        name="layer",
    )(
        *(
            pltpu.with_memory_space_constraint(array, pltpu.HBM)
            for array in (
                jnp.transpose(node_irreps, (1, 2, 0)),
                jnp.transpose(out_grad, (1, 2, 0)),
                edge_source,
                edge_rotation,
                edge_count,
                ghost_slot,
                wigner,
                jnp.transpose(so2_m0, (0, 2, 1, 3)),
                jnp.transpose(so2_m1, (0, 1, 3, 2, 4)),
                jnp.transpose(so2_m2, (0, 1, 3, 2, 4)),
                attn_vector,
            )
        )
    )
    updated = node_irreps.astype(F32) + jnp.transpose(upd, (2, 0, 1))
    irreps_grad = out_grad.astype(F32) + jnp.transpose(grad, (2, 0, 1))
    return updated.astype(BF16), irreps_grad


def solution(mesh):
    placed = (
        P(None, "ch", "dom"),
        P(None, "ch", "dom"),
        P(None, "dom"),
        P(None, "dom"),
        P("dom"),
        P("dom"),
        P(None, "dom"),
        P(None, "ch", None, None),
        P(None, None, "ch", None, None),
        P(None, None, "ch", None, None),
        P("ch"),
    )
    return jax.shard_map(
        on_device,
        mesh=mesh,
        in_specs=placed,
        out_specs=(P(None, "ch", "dom"), P(None, "ch", "dom")),
        check_vma=False,
    )
```

```python
import jax
import jax.numpy as jnp
from jax import lax
from jax.experimental import pallas as pl
from jax.experimental.pallas import tpu as pltpu
from jax.sharding import PartitionSpec as P

LMAX = 6
MMAX = 2
K = 49
OWN = 16
EDGES = 128
KP = 56
ROWS = 2 * KP
PITCH = 116
F32 = jnp.float32
BF16 = jnp.bfloat16
MESH = pl.DeviceIdType.MESH


def rows_of_levels():
    levels = []
    offset = 0
    for level in range(LMAX + 1):
        width = 2 * level + 1
        reach = min(level, MMAX)
        orders = list(range(-reach, reach + 1))
        levels.append((level, width, offset, orders))
        offset += width * width
    return levels


LEVELS = rows_of_levels()


def place(level, order):
    if order == 0:
        return level
    if order == 1:
        return 6 + level
    if order == -1:
        return 12 + level
    if order == 2:
        return 17 + level
    return 22 + level


def iota(shape, dim):
    return lax.broadcasted_iota(jnp.int32, shape, dim)


def one_where(cond):
    return jnp.where(cond, 1.0, 0.0).astype(BF16)


def spin(x, shift):
    return pltpu.roll(x, shift, 1)


def over_slots(x, join):
    parts = [x] + [spin(x, shift) for shift in range(OWN, EDGES, OWN)]
    while len(parts) > 1:
        parts = [join(parts[i], parts[i + 1]) for i in range(0, len(parts), 2)]
    return parts[0]


def dot(a, b):
    return jnp.dot(a, b, preferred_element_type=F32)


def turn(wige, level, width, offset, order, col):
    row = offset + (level + order) * width + col
    return jnp.broadcast_to(wige[row : row + 1, :], (8, EDGES))


def rotate_in(mixed, wige, feats, write):
    groups = range(mixed.shape[0] // ROWS)
    for n in groups:
        for c in range(8):
            feats[n, c * PITCH : c * PITCH + ROWS, :] = mixed[
                n * ROWS : (n + 1) * ROWS, c * EDGES : (c + 1) * EDGES
            ]
    for level, width, offset, orders in LEVELS:
        acc = {}
        for col in range(width):
            k = level * level + col
            parts = [
                feats[n, pl.ds(start + k, 8, stride=PITCH), :] for n in groups for start in (0, KP)
            ]
            for order in orders:
                w = turn(wige, level, width, offset, order, col)
                if col == 0:
                    acc[order] = [w * part for part in parts]
                else:
                    acc[order] = [old + w * part for old, part in zip(acc[order], parts)]
        for order in orders:
            for n in groups:
                write(n, place(level, order), jnp.concatenate(acc[order][2 * n : 2 * n + 2], 0))


def rotate_out(read, wige, back, count):
    for level, width, offset, orders in LEVELS:
        mine = {
            order: [part for n in range(count) for part in read(n, place(level, order))]
            for order in orders
        }
        for col in range(width):
            k = level * level + col
            total = None
            for order in orders:
                w = turn(wige, level, width, offset, order, col)
                if total is None:
                    total = [w * part for part in mine[order]]
                else:
                    total = [old + w * part for old, part in zip(total, mine[order])]
            for n in range(count):
                back[n, pl.ds(k, 8, stride=PITCH), :] = total[2 * n]
                back[n, pl.ds(KP + k, 8, stride=PITCH), :] = total[2 * n + 1]


def across(back, count):
    return jnp.concatenate(
        [
            jnp.concatenate([back[n, c * PITCH : c * PITCH + ROWS, :] for c in range(8)], 1)
            for n in range(count)
        ],
        0,
    )


def to_rows(ref, pad):
    pad[...] = jnp.zeros_like(pad)
    pad[:, 0:K] = ref[...].astype(F32).reshape(256, K)
    low = pad[0:128, :].T
    high = pad[128:256, :].T
    return jnp.concatenate([low[0:KP], high[0:KP]], 0)


def from_rows(rows):
    fill = jnp.zeros((128 - KP, 128), F32)
    low = jnp.concatenate([rows[0:KP], fill], 0).T
    high = jnp.concatenate([rows[KP:ROWS], fill], 0).T
    return jnp.concatenate([low, high], 0)[:, 0:K].reshape(16, 16, K)


def body(
    x_hbm,
    g_hbm,
    src_hbm,
    turn_hbm,
    cnt_hbm,
    slot_hbm,
    wig_hbm,
    w0_hbm,
    w1_hbm,
    w2_hbm,
    attn_hbm,
    upd_ref,
    grad_ref,
    x_ref,
    g_ref,
    src_ref,
    turn_ref,
    cnt_ref,
    slot_ref,
    wig_ref,
    w0_ref,
    w1_ref,
    w2_ref,
    attn_ref,
    load_sem,
    tab,
    pad,
    wige,
    gat,
    sca,
    gat_tile,
    sca_tile,
    feats,
    back,
    rot,
    drot,
    ys,
    ps,
    wt0,
    wt1,
    wt2,
    accum,
    ghost_out,
    from_above,
    from_below,
    x_out,
    x_in,
    z_out,
    z_in,
    red,
    end_x,
    end_sum,
    end_got,
    send_sem,
    tab_sem,
    ghost_send,
    ghost_recv,
    xs_send,
    xs_recv,
    zs_send,
    zs_recv,
    end_send,
    end_recv,
    end_last,
):
    doms = lax.axis_size("dom")
    d = lax.axis_index("dom")
    ch = lax.axis_index("ch")
    zh = ch // 4
    xi = lax.rem(ch, 4)
    mirror = lax.rem(ch + 4, 8)
    up = (lax.rem(d + 1, doms), ch)
    down = (lax.rem(d + doms - 1, doms), ch)
    other = (d, mirror)

    def peer(off):
        return (d, zh * 4 + lax.rem(xi + off, 4))

    has_up = d != doms - 1
    has_down = d != 0
    end = jnp.logical_or(d == 0, d == doms - 1)
    first_end = (doms - 1 - d, ch)
    second_end = (doms - 1 - d, mirror)
    end_in = jnp.where(d == 0, 1, 2)
    end_out = jnp.where(d == 0, 2, 1)
    end_side = jnp.where(d == 0, 0, 1)

    barrier = pltpu.get_barrier_semaphore()

    def greet(target):
        pl.semaphore_signal(barrier, inc=1, device_id=target, device_id_type=MESH)

    for target in (other, peer(1), peer(2), peer(3)):
        greet(target)
    pl.when(has_up)(lambda: greet(up))
    pl.when(has_down)(lambda: greet(down))

    @pl.when(end)
    def _():
        greet(first_end)
        greet(second_end)

    loads = [
        pltpu.make_async_copy(src, dst, load_sem.at[n])
        for n, (src, dst) in enumerate(
            (
                (x_hbm, x_ref),
                (src_hbm, src_ref),
                (turn_hbm, turn_ref),
                (cnt_hbm, cnt_ref),
                (slot_hbm, slot_ref),
                (wig_hbm, wig_ref),
                (g_hbm, g_ref),
                (w0_hbm, w0_ref),
                (w1_hbm, w1_ref),
                (w2_hbm, w2_ref),
                (attn_hbm, attn_ref),
            )
        )
    ]
    for load in loads:
        load.start()
    loads[0].wait()
    tab[0, ch] = to_rows(x_ref, pad).astype(BF16)

    def rcopy(src, dst, ssem, rsem, target):
        return pltpu.make_async_remote_copy(
            src_ref=src,
            dst_ref=dst,
            send_sem=ssem,
            recv_sem=rsem,
            device_id=target,
            device_id_type=MESH,
        )

    def table_copy(blk, who, n, target):
        return rcopy(
            tab.at[0, who], tab.at[blk, who], send_sem.at[n], tab_sem.at[blk, who], target
        )

    def arrival(blk, who):
        return rcopy(
            tab.at[0, who], tab.at[blk, who], send_sem.at[0], tab_sem.at[blk, who], up
        ).wait_recv()

    pl.semaphore_wait(barrier, jnp.where(end, 7, 6))
    sends = []

    def go(blk, who, target, cond=None):
        copy = table_copy(blk, who, len(sends), target)
        if cond is None:
            copy.start()
        else:
            pl.when(cond)(lambda: copy.start())
        sends.append((copy, cond))

    def halo(who):
        go(1, who, up, has_up)
        go(2, who, down, has_down)

    go(0, ch, other)
    go(end_out, ch, second_end, end)
    go(end_out, ch, first_end, end)
    for off in (2, 1, 3):
        go(0, ch, peer(off))
    halo(ch)

    for load in loads[1:6]:
        load.wait()

    spread = one_where(lax.rem(iota((16, EDGES), 1), 16) == iota((16, EDGES), 0))
    pick = (iota((8, EDGES), 1) // 16) == iota((8, EDGES), 0)

    def edge_row(ref):
        wide = dot(ref[...].astype(F32).astype(BF16), spread)
        return jnp.sum(jnp.where(pick, wide, 0.0), axis=0, keepdims=True)

    src = edge_row(src_ref)
    turns = edge_row(turn_ref)
    lane = iota((1, EDGES), 1)
    atom = lax.rem(lane, 16)
    ghost = jnp.zeros((1, EDGES), F32)
    count = jnp.zeros((1, EDGES), jnp.int32)
    for a in range(16):
        ghost = jnp.where(src == 16.0 + a, slot_ref[a].astype(F32), ghost)
        count = jnp.where(atom == a, cnt_ref[a], count)
    nowhere = -1000.0
    index = (
        jnp.where(src < 16.0, src, nowhere),
        jnp.where((src >= 16.0) & (src < 24.0), ghost, nowhere),
        jnp.where(src >= 24.0, ghost, nowhere),
    )
    row_id = iota((EDGES, EDGES), 0).astype(F32)
    lane_id = iota((EDGES, EDGES), 1).astype(F32)
    for blk in range(4):
        idx = atom.astype(F32) if blk == 3 else index[blk]
        wide = jnp.broadcast_to(idx, (EDGES, EDGES))
        tall = wide.T
        for c in range(8):
            forth = one_where(row_id == wide + 16.0 * c)
            fro = one_where(lane_id == tall + 16.0 * c)
            if blk == 3:
                gat_tile[:, c * 128 : c * 128 + 128] = forth
                sca_tile[c * 128 : c * 128 + 128, :] = fro
            else:
                gat[blk * 128 : blk * 128 + 128, c * 128 : c * 128 + 128] = forth
                sca[c * 128 : c * 128 + 128, blk * 128 : blk * 128 + 128] = fro

    chosen = one_where(iota((256, EDGES), 0).astype(F32) == jnp.broadcast_to(turns, (256, EDGES)))
    whole = wig_ref[...]
    first = whole.astype(BF16)
    rest = whole - first.astype(F32)
    second = rest.astype(BF16)
    third = (rest - second.astype(F32)).astype(BF16)
    wige[...] = dot(first, chosen) + (dot(second, chosen) + dot(third, chosen))

    for load in loads[6:]:
        load.wait()

    def keep_p(n, pos, value):
        ps[pos] = value

    rotate_in(dot(to_rows(g_ref, pad).astype(BF16), gat_tile[...]), wige, feats, keep_p)

    for lev in range(7):
        tile = w0_ref[:, lev].reshape(112, 128).astype(F32)
        wt0[lev * 128 : lev * 128 + 128, :] = (
            jnp.concatenate([tile, jnp.zeros((16, 128), F32)], 0).T.astype(BF16)
        )
    for ref, out, n in ((w1_ref, wt1, 6), (w2_ref, wt2, 5)):
        for part in range(2):
            for lev in range(n):
                tile = ref[part, :, lev].reshape(n * 16, 128).astype(F32)
                tile = jnp.concatenate([tile, jnp.zeros((128 - n * 16, 128), F32)], 0)
                out[lev * 128 : lev * 128 + 128, part * 128 : part * 128 + 128] = (
                    tile.T.astype(BF16)
                )
    back[...] = jnp.zeros_like(back)

    near = [zh * 4 + lax.rem(xi + off, 4) for off in (1, 3, 2)]
    far = [(1 - zh) * 4 + lax.rem(xi + off, 4) for off in (1, 3, 2)]
    arrival(0, near[0])
    halo(near[0])
    arrival(0, near[1])
    halo(near[1])
    arrival(0, near[2])
    halo(near[2])

    def end_copy(n, who, target):
        return rcopy(
            tab.at[end_in, who],
            tab.at[end_in, who],
            end_send.at[n],
            tab_sem.at[end_in, who],
            target,
        )

    @pl.when(end)
    def _():
        for n, who in enumerate((mirror, ch)):
            end_copy(0, who, first_end).wait_recv()
            for j, off in enumerate((2, 1, 3)):
                end_copy(n * 3 + j, who, peer(off)).start()

    arrival(0, mirror)
    for off in (2, 1, 3):
        go(0, mirror, peer(off))
    halo(mirror)
    for who in far:
        arrival(0, who)
        halo(who)

    def halo_arrival(blk, who):
        came = jnp.logical_and(end, jnp.logical_and(lax.rem(who, 4) == xi, blk == end_in))
        pl.when(jnp.logical_not(came))(lambda: arrival(blk, who))

    def pair_in(i, carry):
        side = lax.rem(zh + i // 2, 2)
        both = [side * 4 + lax.rem(xi + lax.rem(2 * i, 4) + n, 4) for n in range(2)]
        for who in both:
            halo_arrival(1, who)
            halo_arrival(2, who)
        lhs = jnp.concatenate(
            [jnp.concatenate([tab[0, who], tab[1, who], tab[2, who]], 1) for who in both], 0
        )

        def keep(n, pos, value):
            rot[pl.ds(pl.multiple_of(pos * 128 + both[n] * 16, 16), 16), :] = value.astype(BF16)

        rotate_in(dot(lhs, gat[...]), wige, feats, keep)
        return carry

    lax.fori_loop(0, 4, pair_in, 0)
    w0 = jnp.concatenate([w0_ref[:, lev].reshape(112, 128) for lev in range(7)], 1)
    y0 = dot(w0, rot[0:896, :])
    ys[0:7] = y0.reshape(7, 16, EDGES)
    for ref, n, start in ((w1_ref, 6, 7), (w2_ref, 5, 19)):
        lhs = jnp.concatenate(
            [ref[:, :, lev].reshape(2 * n * 16, 128) for lev in range(n)], 1
        )
        plus = rot[start * 128 : (start + n) * 128, :]
        minus = rot[(start + n) * 128 : (start + 2 * n) * 128, :]
        both = dot(lhs, jnp.concatenate([plus, minus], 1))
        half = n * 16
        ys[start : start + n] = (both[:half, :128] - both[half:, 128:]).reshape(n, 16, EDGES)
        ys[start + n : start + 2 * n] = (both[:half, 128:] + both[half:, :128]).reshape(
            n, 16, EDGES
        )

    attn = jnp.zeros((16, EDGES), F32)
    rows = iota((16, EDGES), 0)
    for t in range(16):
        attn = jnp.where(rows == t, attn_ref[t], attn)
    scalar = ys[0]
    gate = jax.nn.sigmoid(scalar)
    score = jnp.sum(scalar * gate * attn, axis=0, keepdims=True)
    live = jnp.broadcast_to((lane // 16) < count, (8, EDGES))
    score = jnp.broadcast_to(score, (8, EDGES))
    masked = jnp.where(live, score, -1e30)
    top = over_slots(masked, jnp.maximum)
    weight = jnp.exp(jnp.where(live, score - top, -1e30))
    weight = weight / over_slots(weight, jnp.add)
    weight2 = jnp.concatenate([weight, weight], 0)
    inner = ys[0] * ps[0]
    for pos in range(1, 29):
        inner = inner + ys[pos] * ps[pos]
    dweight = jnp.broadcast_to(jnp.sum(inner * gate, axis=0, keepdims=True), (8, EDGES))
    mean = over_slots(weight * dweight, jnp.add)
    dscore = weight * (dweight - mean)
    dscore2 = jnp.concatenate([dscore, dscore], 0)
    slope = gate * (1.0 - gate)
    dscalar = weight2 * inner * slope + dscore2 * attn * (gate + scalar * slope)
    factor = weight2 * gate

    nil = jnp.zeros((16, EDGES), F32)
    gated = [ps[pos] * gate for pos in range(29)]
    for out, n, start in ((wt1, 6, 7), (wt2, 5, 19)):
        plus = jnp.concatenate(gated[start : start + n] + [nil] * (8 - n), 0).astype(BF16)
        minus = jnp.concatenate(gated[start + n : start + 2 * n] + [nil] * (8 - n), 0).astype(BF16)
        rhs = jnp.concatenate(
            [jnp.concatenate([plus, minus], 1), jnp.concatenate([minus, -plus], 1)], 0
        )
        both = dot(out[...], rhs)
        tall = jnp.broadcast_to(weight[0:1], (n * 128, EDGES))
        drot[start * 128 : (start + n) * 128, :] = (both[:, :128] * tall).astype(BF16)
        drot[(start + n) * 128 : (start + 2 * n) * 128, :] = (both[:, 128:] * tall).astype(BF16)
    dys = [gated[pos] * weight2 for pos in range(7)]
    dys[0] = dys[0] + dscalar
    dy0 = jnp.concatenate(dys + [nil], 0).astype(BF16)
    drot[0:896, :] = dot(wt0[...], dy0).astype(BF16)

    def group_of(i):
        half = i // 4
        j = lax.rem(i, 4)
        off = jnp.where(j == 0, 2, jnp.where(j == 1, 1, jnp.where(j == 2, 3, 0)))
        return lax.rem(1 - zh + half, 2) * 4 + lax.rem(xi + off, 4)

    def to_down(who):
        return rcopy(
            ghost_out.at[0, who],
            from_above.at[who],
            ghost_send.at[0, who],
            ghost_recv.at[0, who],
            down,
        )

    def to_up(who):
        return rcopy(
            ghost_out.at[1, who],
            from_below.at[who],
            ghost_send.at[1, who],
            ghost_recv.at[1, who],
            up,
        )

    offs = (2, 1, 3)

    def end_part(i, who, target):
        return rcopy(
            ghost_out.at[end_side, who], end_x.at[i], end_send.at[i], end_recv.at[i], target
        )

    def end_peer(i):
        half = i // 3
        off = offs[i % 3]
        who = ((zh + 1 - half) % 2) * 4 + lax.rem(xi + off, 4)
        return end_part(i, who, peer(off))

    def pair_out(step, carry):
        i = lax.rem(step + jnp.where(d == doms - 1, 2, 0), 4)
        both = [group_of(2 * i + n) for n in range(2)]

        def read(n, pos):
            start = pl.multiple_of(pos * 128 + both[n] * 16, 16)
            value = drot[pl.ds(start, 16), :].astype(F32)
            return value[0:8], value[8:16]

        rotate_out(read, wige, back, 2)
        out = dot(across(back, 2).astype(BF16), sca[...])
        for n, who in enumerate(both):
            part = out[n * ROWS : (n + 1) * ROWS]
            ghost_out[0, who] = part[:, 128:256].astype(BF16)
            ghost_out[1, who] = part[:, 256:384].astype(BF16)
            pl.when(has_down)(lambda who=who: to_down(who).start())
            pl.when(has_up)(lambda who=who: to_up(who).start())
            accum[who] = part[:, 0:128]

        odd = lax.rem(i, 2)

        @pl.when(end)
        def _():
            end_part((i // 2) * 3 + odd * 2, both[0], peer(2 + odd)).start()

        @pl.when(jnp.logical_and(end, odd == 0))
        def _():
            end_part((i // 2) * 3 + 1, both[1], peer(1)).start()

        return carry

    @pl.when(d == doms - 1)
    def _():
        from_above[...] = jnp.zeros_like(from_above)

    @pl.when(d == 0)
    def _():
        from_below[...] = jnp.zeros_like(from_below)

    lax.fori_loop(0, 4, pair_out, 0)

    def end_home(half):
        target = (second_end, first_end)[half]
        return rcopy(
            end_sum.at[half], end_got.at[half], end_last.at[half], end_last.at[2 + half], target
        )


    def to_peer(i, off):
        return rcopy(x_out.at[i], x_in.at[i], xs_send.at[i], xs_recv.at[i], peer(off))

    def finish(i):
        who = group_of(i)
        pl.when(has_up)(lambda: to_down(who).wait_recv())
        pl.when(has_down)(lambda: to_up(who).wait_recv())
        return accum[who] + from_above[who].astype(F32) + from_below[who].astype(F32)

    def along_x(half):
        for j in range(3):
            x_out[half * 3 + j] = finish(half * 4 + j).astype(BF16)
            to_peer(half * 3 + j, offs[j]).start()
        red[half] = finish(half * 4 + 3)

    along_x(0)

    def gathered(half):
        total = red[half]
        for j in range(3):
            to_peer(half * 3 + j, offs[j]).wait_recv()
            total = total + x_in[half * 3 + j].astype(F32)
        return total

    @pl.when(end)
    def _():
        for half in (1, 0):
            who = ((zh + 1 - half) % 2) * 4 + xi
            total = ghost_out[end_side, who].astype(F32)
            for j in range(3):
                end_peer(half * 3 + j).wait_recv()
                total = total + end_x[half * 3 + j].astype(F32)
            end_sum[half] = total.astype(BF16)
            end_home(half).start()

    z_out[...] = gathered(0).astype(BF16)
    across_z = rcopy(z_out, z_in, zs_send.at[0], zs_recv.at[0], other)
    across_z.start()
    along_x(1)

    def read_z(n, pos):
        value = ys[pos] * factor
        return value[0:8], value[8:16]

    rotate_out(read_z, wige, back, 1)
    wide = across(back, 1)
    first = wide.astype(BF16)
    second = (wide - first.astype(F32)).astype(BF16)
    agg = dot(first, sca_tile[...]) + dot(second, sca_tile[...])
    upd_ref[...] = from_rows(agg)

    red[1] = gathered(1)

    @pl.when(end)
    def _():
        end_home(0).wait_recv()
        end_home(1).wait_recv()
        red[1] = red[1] + (end_got[0].astype(F32) + end_got[1].astype(F32))

    for i in range(6):
        to_peer(i, offs[i % 3]).wait_send()
    for i in range(8):
        pl.when(has_down)(lambda i=i: to_down(i).wait_send())
        pl.when(has_up)(lambda i=i: to_up(i).wait_send())

    @pl.when(end)
    def _():
        for i in range(6):
            end_peer(i).wait_send()
        end_home(0).wait_send()
        end_home(1).wait_send()
    for copy, cond in sends:
        if cond is None:
            copy.wait_send()
        else:
            pl.when(cond)(lambda copy=copy: copy.wait_send())

    @pl.when(end)
    def _():
        for n, who in enumerate((mirror, ch)):
            for j, off in enumerate((2, 1, 3)):
                end_copy(n * 3 + j, who, peer(off)).wait_send()
    across_z.wait_send()
    across_z.wait_recv()
    grad = red[1] + z_in[...].astype(F32)
    grad_ref[...] = from_rows(grad)


def on_device(
    node_irreps,
    out_grad,
    edge_source,
    edge_rotation,
    edge_count,
    ghost_slot,
    wigner,
    so2_m0,
    so2_m1,
    so2_m2,
    attn_vector,
):
    vmem = pl.BlockSpec(memory_space=pltpu.VMEM)
    hbm = pl.BlockSpec(memory_space=pltpu.HBM)
    block = (ROWS, 128)
    dma = pltpu.SemaphoreType.DMA
    upd, grad = pl.pallas_call(
        body,
        out_shape=(
            jax.ShapeDtypeStruct((16, 16, K), F32),
            jax.ShapeDtypeStruct((16, 16, K), F32),
        ),
        in_specs=[hbm] * 11,
        out_specs=(vmem, vmem),
        scratch_shapes=[
            pltpu.VMEM((16, 16, K), BF16),
            pltpu.VMEM((16, 16, K), BF16),
            pltpu.VMEM((8, 16), jnp.int32),
            pltpu.VMEM((8, 16), jnp.int32),
            pltpu.SMEM((16,), jnp.int32),
            pltpu.SMEM((16,), jnp.int32),
            pltpu.VMEM((455, 256), F32),
            pltpu.VMEM((7, 7, 16, 128), BF16),
            pltpu.VMEM((2, 6, 6, 16, 128), BF16),
            pltpu.VMEM((2, 5, 5, 16, 128), BF16),
            pltpu.SMEM((16,), F32),
            dma((11,)),
            pltpu.VMEM((3, 8) + block, BF16),
            pltpu.VMEM((256, 128), F32),
            pltpu.VMEM((455, EDGES), F32),
            pltpu.VMEM((384, 1024), BF16),
            pltpu.VMEM((1024, 384), BF16),
            pltpu.VMEM((128, 1024), BF16),
            pltpu.VMEM((1024, 128), BF16),
            pltpu.VMEM((2, 8 * PITCH, 128), F32),
            pltpu.VMEM((2, 8 * PITCH, 128), F32),
            pltpu.VMEM((29 * 128, EDGES), BF16),
            pltpu.VMEM((29 * 128, EDGES), BF16),
            pltpu.VMEM((29, 16, EDGES), F32),
            pltpu.VMEM((29, 16, EDGES), F32),
            pltpu.VMEM((896, 128), BF16),
            pltpu.VMEM((768, 256), BF16),
            pltpu.VMEM((640, 256), BF16),
            pltpu.VMEM((8,) + block, F32),
            pltpu.VMEM((2, 8) + block, BF16),
            pltpu.VMEM((8,) + block, BF16),
            pltpu.VMEM((8,) + block, BF16),
            pltpu.VMEM((6,) + block, BF16),
            pltpu.VMEM((6,) + block, BF16),
            pltpu.VMEM(block, BF16),
            pltpu.VMEM(block, BF16),
            pltpu.VMEM((2,) + block, F32),
            pltpu.VMEM((6,) + block, BF16),
            pltpu.VMEM((2,) + block, BF16),
            pltpu.VMEM((2,) + block, BF16),
            dma((27,)),
            dma((3, 8)),
            dma((2, 8)),
            dma((2, 8)),
            dma((6,)),
            dma((6,)),
            dma((1,)),
            dma((1,)),
            dma((6,)),
            dma((6,)),
            dma((4,)),
        ],
        compiler_params=pltpu.CompilerParams(
            collective_id=0, has_side_effects=True, vmem_limit_bytes=24 * 1024 * 1024
        ),
        name="layer",
    )(
        *(
            pltpu.with_memory_space_constraint(array, pltpu.HBM)
            for array in (
                jnp.transpose(node_irreps, (1, 2, 0)),
                jnp.transpose(out_grad, (1, 2, 0)),
                edge_source,
                edge_rotation,
                edge_count,
                ghost_slot,
                wigner,
                jnp.transpose(so2_m0, (0, 2, 1, 3)),
                jnp.transpose(so2_m1, (0, 1, 3, 2, 4)),
                jnp.transpose(so2_m2, (0, 1, 3, 2, 4)),
                attn_vector,
            )
        )
    )
    updated = node_irreps.astype(F32) + jnp.transpose(upd, (2, 0, 1))
    irreps_grad = out_grad.astype(F32) + jnp.transpose(grad, (2, 0, 1))
    return updated.astype(BF16), irreps_grad


def solution(mesh):
    placed = (
        P(None, "ch", "dom"),
        P(None, "ch", "dom"),
        P(None, "dom"),
        P(None, "dom"),
        P("dom"),
        P("dom"),
        P(None, "dom"),
        P(None, "ch", None, None),
        P(None, None, "ch", None, None),
        P(None, None, "ch", None, None),
        P("ch"),
    )
    return jax.shard_map(
        on_device,
        mesh=mesh,
        in_specs=placed,
        out_specs=(P(None, "ch", "dom"), P(None, "ch", "dom")),
        check_vma=False,
    )
```

```python
import jax
import jax.numpy as jnp
from jax import lax
from jax.experimental import pallas as pl
from jax.experimental.pallas import tpu as pltpu
from jax.sharding import PartitionSpec as P

LMAX = 6
MMAX = 2
K = 49
OWN = 16
EDGES = 128
KP = 56
ROWS = 2 * KP
PITCH = 116
F32 = jnp.float32
BF16 = jnp.bfloat16
MESH = pl.DeviceIdType.MESH


def rows_of_levels():
    levels = []
    offset = 0
    for level in range(LMAX + 1):
        width = 2 * level + 1
        reach = min(level, MMAX)
        orders = list(range(-reach, reach + 1))
        levels.append((level, width, offset, orders))
        offset += width * width
    return levels


LEVELS = rows_of_levels()


def place(level, order):
    if order == 0:
        return level
    if order == 1:
        return 6 + level
    if order == -1:
        return 12 + level
    if order == 2:
        return 17 + level
    return 22 + level


def iota(shape, dim):
    return lax.broadcasted_iota(jnp.int32, shape, dim)


def one_where(cond):
    return jnp.where(cond, 1.0, 0.0).astype(BF16)


def spin(x, shift):
    return pltpu.roll(x, shift, 1)


def over_slots(x, join):
    parts = [x] + [spin(x, shift) for shift in range(OWN, EDGES, OWN)]
    while len(parts) > 1:
        parts = [join(parts[i], parts[i + 1]) for i in range(0, len(parts), 2)]
    return parts[0]


def dot(a, b):
    return jnp.dot(a, b, preferred_element_type=F32)


def turn(wige, level, width, offset, order, col):
    row = offset + (level + order) * width + col
    return jnp.broadcast_to(wige[row : row + 1, :], (8, EDGES))


def rotate_in(mixed, wige, feats, write):
    groups = range(mixed.shape[0] // ROWS)
    for n in groups:
        for c in range(8):
            feats[n, c * PITCH : c * PITCH + ROWS, :] = mixed[
                n * ROWS : (n + 1) * ROWS, c * EDGES : (c + 1) * EDGES
            ]
    for level, width, offset, orders in LEVELS:
        acc = {}
        for col in range(width):
            k = level * level + col
            parts = [
                feats[n, pl.ds(start + k, 8, stride=PITCH), :] for n in groups for start in (0, KP)
            ]
            for order in orders:
                w = turn(wige, level, width, offset, order, col)
                if col == 0:
                    acc[order] = [w * part for part in parts]
                else:
                    acc[order] = [old + w * part for old, part in zip(acc[order], parts)]
        for order in orders:
            for n in groups:
                write(n, place(level, order), jnp.concatenate(acc[order][2 * n : 2 * n + 2], 0))


def rotate_out(read, wige, back, count):
    for level, width, offset, orders in LEVELS:
        mine = {
            order: [part for n in range(count) for part in read(n, place(level, order))]
            for order in orders
        }
        for col in range(width):
            k = level * level + col
            total = None
            for order in orders:
                w = turn(wige, level, width, offset, order, col)
                if total is None:
                    total = [w * part for part in mine[order]]
                else:
                    total = [old + w * part for old, part in zip(total, mine[order])]
            for n in range(count):
                back[n, pl.ds(k, 8, stride=PITCH), :] = total[2 * n]
                back[n, pl.ds(KP + k, 8, stride=PITCH), :] = total[2 * n + 1]


def across(back, count):
    return jnp.concatenate(
        [
            jnp.concatenate([back[n, c * PITCH : c * PITCH + ROWS, :] for c in range(8)], 1)
            for n in range(count)
        ],
        0,
    )


def to_rows(ref, pad):
    pad[...] = jnp.zeros_like(pad)
    pad[:, 0:K] = ref[...].astype(F32).reshape(256, K)
    low = pad[0:128, :].T
    high = pad[128:256, :].T
    return jnp.concatenate([low[0:KP], high[0:KP]], 0)


def from_rows(rows):
    fill = jnp.zeros((128 - KP, 128), F32)
    low = jnp.concatenate([rows[0:KP], fill], 0).T
    high = jnp.concatenate([rows[KP:ROWS], fill], 0).T
    return jnp.concatenate([low, high], 0)[:, 0:K].reshape(16, 16, K)


def body(
    x_hbm,
    g_hbm,
    src_hbm,
    turn_hbm,
    cnt_hbm,
    slot_hbm,
    wig_hbm,
    w0_hbm,
    w1_hbm,
    w2_hbm,
    attn_hbm,
    upd_ref,
    grad_ref,
    x_ref,
    g_ref,
    src_ref,
    turn_ref,
    cnt_ref,
    slot_ref,
    wig_ref,
    w0_ref,
    w1_ref,
    w2_ref,
    attn_ref,
    load_sem,
    tab,
    pad,
    wige,
    gat,
    sca,
    gat_tile,
    sca_tile,
    feats,
    back,
    rot,
    drot,
    ys,
    ps,
    wt0,
    wt1,
    wt2,
    accum,
    ghost_out,
    from_above,
    from_below,
    x_out,
    x_in,
    z_out,
    z_in,
    red,
    end_x,
    end_sum,
    end_got,
    send_sem,
    tab_sem,
    ghost_send,
    ghost_recv,
    xs_send,
    xs_recv,
    zs_send,
    zs_recv,
    end_send,
    end_recv,
    end_last,
):
    doms = lax.axis_size("dom")
    d = lax.axis_index("dom")
    ch = lax.axis_index("ch")
    zh = ch // 4
    xi = lax.rem(ch, 4)
    mirror = lax.rem(ch + 4, 8)
    up = (lax.rem(d + 1, doms), ch)
    down = (lax.rem(d + doms - 1, doms), ch)
    other = (d, mirror)

    def peer(off):
        return (d, zh * 4 + lax.rem(xi + off, 4))

    has_up = d != doms - 1
    has_down = d != 0
    end = jnp.logical_or(d == 0, d == doms - 1)
    first_end = (doms - 1 - d, ch)
    second_end = (doms - 1 - d, mirror)
    end_in = jnp.where(d == 0, 1, 2)
    end_out = jnp.where(d == 0, 2, 1)
    end_side = jnp.where(d == 0, 0, 1)

    barrier = pltpu.get_barrier_semaphore()

    def greet(target):
        pl.semaphore_signal(barrier, inc=1, device_id=target, device_id_type=MESH)

    for target in (other, peer(1), peer(2), peer(3)):
        greet(target)
    pl.when(has_up)(lambda: greet(up))
    pl.when(has_down)(lambda: greet(down))

    @pl.when(end)
    def _():
        greet(first_end)
        greet(second_end)

    loads = [
        pltpu.make_async_copy(src, dst, load_sem.at[n])
        for n, (src, dst) in enumerate(
            (
                (x_hbm, x_ref),
                (src_hbm, src_ref),
                (turn_hbm, turn_ref),
                (cnt_hbm, cnt_ref),
                (slot_hbm, slot_ref),
                (wig_hbm, wig_ref),
                (g_hbm, g_ref),
                (w0_hbm, w0_ref),
                (w1_hbm, w1_ref),
                (w2_hbm, w2_ref),
                (attn_hbm, attn_ref),
            )
        )
    ]
    for load in loads:
        load.start()
    loads[0].wait()
    tab[0, ch] = to_rows(x_ref, pad).astype(BF16)

    def rcopy(src, dst, ssem, rsem, target):
        return pltpu.make_async_remote_copy(
            src_ref=src,
            dst_ref=dst,
            send_sem=ssem,
            recv_sem=rsem,
            device_id=target,
            device_id_type=MESH,
        )

    def table_copy(blk, who, n, target):
        return rcopy(
            tab.at[0, who], tab.at[blk, who], send_sem.at[n], tab_sem.at[blk, who], target
        )

    def arrival(blk, who):
        return rcopy(
            tab.at[0, who], tab.at[blk, who], send_sem.at[0], tab_sem.at[blk, who], up
        ).wait_recv()

    pl.semaphore_wait(barrier, jnp.where(end, 7, 6))
    sends = []

    def go(blk, who, target, cond=None):
        copy = table_copy(blk, who, len(sends), target)
        if cond is None:
            copy.start()
        else:
            pl.when(cond)(lambda: copy.start())
        sends.append((copy, cond))

    def halo(who):
        go(1, who, up, has_up)
        go(2, who, down, has_down)

    go(0, ch, other)
    go(end_out, ch, second_end, end)
    go(end_out, ch, first_end, end)
    for off in (2, 1, 3):
        go(0, ch, peer(off))
    halo(ch)

    for load in loads[1:6]:
        load.wait()

    spread = one_where(lax.rem(iota((16, EDGES), 1), 16) == iota((16, EDGES), 0))
    pick = (iota((8, EDGES), 1) // 16) == iota((8, EDGES), 0)

    def edge_row(ref):
        wide = dot(ref[...].astype(F32).astype(BF16), spread)
        return jnp.sum(jnp.where(pick, wide, 0.0), axis=0, keepdims=True)

    src = edge_row(src_ref)
    turns = edge_row(turn_ref)
    lane = iota((1, EDGES), 1)
    atom = lax.rem(lane, 16)
    ghost = jnp.zeros((1, EDGES), F32)
    count = jnp.zeros((1, EDGES), jnp.int32)
    for a in range(16):
        ghost = jnp.where(src == 16.0 + a, slot_ref[a].astype(F32), ghost)
        count = jnp.where(atom == a, cnt_ref[a], count)
    nowhere = -1000.0
    index = (
        jnp.where(src < 16.0, src, nowhere),
        jnp.where((src >= 16.0) & (src < 24.0), ghost, nowhere),
        jnp.where(src >= 24.0, ghost, nowhere),
    )
    row_id = iota((EDGES, EDGES), 0).astype(F32)
    lane_id = iota((EDGES, EDGES), 1).astype(F32)
    for blk in range(4):
        idx = atom.astype(F32) if blk == 3 else index[blk]
        wide = jnp.broadcast_to(idx, (EDGES, EDGES))
        tall = wide.T
        for c in range(8):
            forth = one_where(row_id == wide + 16.0 * c)
            fro = one_where(lane_id == tall + 16.0 * c)
            if blk == 3:
                gat_tile[:, c * 128 : c * 128 + 128] = forth
                sca_tile[c * 128 : c * 128 + 128, :] = fro
            else:
                gat[blk * 128 : blk * 128 + 128, c * 128 : c * 128 + 128] = forth
                sca[c * 128 : c * 128 + 128, blk * 128 : blk * 128 + 128] = fro

    chosen = one_where(iota((256, EDGES), 0).astype(F32) == jnp.broadcast_to(turns, (256, EDGES)))
    whole = wig_ref[...]
    first = whole.astype(BF16)
    rest = whole - first.astype(F32)
    second = rest.astype(BF16)
    third = (rest - second.astype(F32)).astype(BF16)
    wige[...] = dot(first, chosen) + (dot(second, chosen) + dot(third, chosen))

    for load in loads[6:]:
        load.wait()

    def keep_p(n, pos, value):
        ps[pos] = value

    rotate_in(dot(to_rows(g_ref, pad).astype(BF16), gat_tile[...]), wige, feats, keep_p)

    for lev in range(7):
        tile = w0_ref[:, lev].reshape(112, 128).astype(F32)
        wt0[lev * 128 : lev * 128 + 128, :] = (
            jnp.concatenate([tile, jnp.zeros((16, 128), F32)], 0).T.astype(BF16)
        )
    for ref, out, n in ((w1_ref, wt1, 6), (w2_ref, wt2, 5)):
        for part in range(2):
            for lev in range(n):
                tile = ref[part, :, lev].reshape(n * 16, 128).astype(F32)
                tile = jnp.concatenate([tile, jnp.zeros((128 - n * 16, 128), F32)], 0)
                out[lev * 128 : lev * 128 + 128, part * 128 : part * 128 + 128] = (
                    tile.T.astype(BF16)
                )
    back[...] = jnp.zeros_like(back)

    near = [zh * 4 + lax.rem(xi + off, 4) for off in (1, 3, 2)]
    far = [(1 - zh) * 4 + lax.rem(xi + off, 4) for off in (1, 3, 2)]
    arrival(0, near[0])
    halo(near[0])
    arrival(0, near[1])
    halo(near[1])
    arrival(0, near[2])
    halo(near[2])

    def end_copy(n, who, target):
        return rcopy(
            tab.at[end_in, who],
            tab.at[end_in, who],
            end_send.at[n],
            tab_sem.at[end_in, who],
            target,
        )

    @pl.when(end)
    def _():
        for n, who in enumerate((mirror, ch)):
            end_copy(0, who, first_end).wait_recv()
            for j, off in enumerate((2, 1, 3)):
                end_copy(n * 3 + j, who, peer(off)).start()

    arrival(0, mirror)
    for off in (2, 1, 3):
        go(0, mirror, peer(off))
    halo(mirror)
    for who in far:
        arrival(0, who)
        halo(who)

    def halo_arrival(blk, who):
        came = jnp.logical_and(end, jnp.logical_and(lax.rem(who, 4) == xi, blk == end_in))
        pl.when(jnp.logical_not(came))(lambda: arrival(blk, who))

    def pair_in(i, carry):
        side = lax.rem(zh + i // 2, 2)
        both = [side * 4 + lax.rem(xi + lax.rem(2 * i, 4) + n, 4) for n in range(2)]
        for who in both:
            halo_arrival(1, who)
            halo_arrival(2, who)
        lhs = jnp.concatenate(
            [jnp.concatenate([tab[0, who], tab[1, who], tab[2, who]], 1) for who in both], 0
        )

        def keep(n, pos, value):
            rot[pl.ds(pl.multiple_of(pos * 128 + both[n] * 16, 16), 16), :] = value.astype(BF16)

        rotate_in(dot(lhs, gat[...]), wige, feats, keep)
        return carry

    lax.fori_loop(0, 4, pair_in, 0)
    w0 = jnp.concatenate([w0_ref[:, lev].reshape(112, 128) for lev in range(7)], 1)
    y0 = dot(w0, rot[0:896, :])
    ys[0:7] = y0.reshape(7, 16, EDGES)
    for ref, n, start in ((w1_ref, 6, 7), (w2_ref, 5, 19)):
        lhs = jnp.concatenate(
            [ref[:, :, lev].reshape(2 * n * 16, 128) for lev in range(n)], 1
        )
        plus = rot[start * 128 : (start + n) * 128, :]
        minus = rot[(start + n) * 128 : (start + 2 * n) * 128, :]
        both = dot(lhs, jnp.concatenate([plus, minus], 1))
        half = n * 16
        ys[start : start + n] = (both[:half, :128] - both[half:, 128:]).reshape(n, 16, EDGES)
        ys[start + n : start + 2 * n] = (both[:half, 128:] + both[half:, :128]).reshape(
            n, 16, EDGES
        )

    attn = jnp.zeros((16, EDGES), F32)
    rows = iota((16, EDGES), 0)
    for t in range(16):
        attn = jnp.where(rows == t, attn_ref[t], attn)
    scalar = ys[0]
    gate = jax.nn.sigmoid(scalar)
    score = jnp.sum(scalar * gate * attn, axis=0, keepdims=True)
    live = jnp.broadcast_to((lane // 16) < count, (8, EDGES))
    score = jnp.broadcast_to(score, (8, EDGES))
    masked = jnp.where(live, score, -1e30)
    top = over_slots(masked, jnp.maximum)
    weight = jnp.exp(jnp.where(live, score - top, -1e30))
    weight = weight / over_slots(weight, jnp.add)
    weight2 = jnp.concatenate([weight, weight], 0)
    inner = ys[0] * ps[0]
    for pos in range(1, 29):
        inner = inner + ys[pos] * ps[pos]
    dweight = jnp.broadcast_to(jnp.sum(inner * gate, axis=0, keepdims=True), (8, EDGES))
    mean = over_slots(weight * dweight, jnp.add)
    dscore = weight * (dweight - mean)
    dscore2 = jnp.concatenate([dscore, dscore], 0)
    slope = gate * (1.0 - gate)
    dscalar = weight2 * inner * slope + dscore2 * attn * (gate + scalar * slope)
    factor = weight2 * gate

    nil = jnp.zeros((16, EDGES), F32)
    gated = [ps[pos] * gate for pos in range(29)]
    for out, n, start in ((wt1, 6, 7), (wt2, 5, 19)):
        plus = jnp.concatenate(gated[start : start + n] + [nil] * (8 - n), 0).astype(BF16)
        minus = jnp.concatenate(gated[start + n : start + 2 * n] + [nil] * (8 - n), 0).astype(BF16)
        rhs = jnp.concatenate(
            [jnp.concatenate([plus, minus], 1), jnp.concatenate([minus, -plus], 1)], 0
        )
        both = dot(out[...], rhs)
        tall = jnp.broadcast_to(weight[0:1], (n * 128, EDGES))
        drot[start * 128 : (start + n) * 128, :] = (both[:, :128] * tall).astype(BF16)
        drot[(start + n) * 128 : (start + 2 * n) * 128, :] = (both[:, 128:] * tall).astype(BF16)
    dys = [gated[pos] * weight2 for pos in range(7)]
    dys[0] = dys[0] + dscalar
    dy0 = jnp.concatenate(dys + [nil], 0).astype(BF16)
    drot[0:896, :] = dot(wt0[...], dy0).astype(BF16)

    def group_of(i):
        half = i // 4
        j = lax.rem(i, 4)
        off = jnp.where(j == 0, 2, jnp.where(j == 1, 1, jnp.where(j == 2, 3, 0)))
        return lax.rem(1 - zh + half, 2) * 4 + lax.rem(xi + off, 4)

    def to_down(who):
        return rcopy(
            ghost_out.at[0, who],
            from_above.at[who],
            ghost_send.at[0, who],
            ghost_recv.at[0, who],
            down,
        )

    def to_up(who):
        return rcopy(
            ghost_out.at[1, who],
            from_below.at[who],
            ghost_send.at[1, who],
            ghost_recv.at[1, who],
            up,
        )

    offs = (2, 1, 3)

    def end_part(i, who, target):
        return rcopy(
            ghost_out.at[end_side, who], end_x.at[i], end_send.at[i], end_recv.at[i], target
        )

    def end_peer(i):
        half = i // 3
        off = offs[i % 3]
        who = ((zh + 1 - half) % 2) * 4 + lax.rem(xi + off, 4)
        return end_part(i, who, peer(off))

    def pair_out(step, carry):
        i = lax.rem(step + jnp.where(d == doms - 1, 2, 0), 4)
        both = [group_of(2 * i + n) for n in range(2)]

        def read(n, pos):
            start = pl.multiple_of(pos * 128 + both[n] * 16, 16)
            value = drot[pl.ds(start, 16), :].astype(F32)
            return value[0:8], value[8:16]

        rotate_out(read, wige, back, 2)
        out = dot(across(back, 2).astype(BF16), sca[...])
        for n, who in enumerate(both):
            part = out[n * ROWS : (n + 1) * ROWS]
            ghost_out[0, who] = part[:, 128:256].astype(BF16)
            ghost_out[1, who] = part[:, 256:384].astype(BF16)
            pl.when(has_down)(lambda who=who: to_down(who).start())
            pl.when(has_up)(lambda who=who: to_up(who).start())
            accum[who] = part[:, 0:128]

        odd = lax.rem(i, 2)

        @pl.when(end)
        def _():
            end_part((i // 2) * 3 + odd * 2, both[0], peer(2 + odd)).start()

        @pl.when(jnp.logical_and(end, odd == 0))
        def _():
            end_part((i // 2) * 3 + 1, both[1], peer(1)).start()

        return carry

    @pl.when(d == doms - 1)
    def _():
        from_above[...] = jnp.zeros_like(from_above)

    @pl.when(d == 0)
    def _():
        from_below[...] = jnp.zeros_like(from_below)

    lax.fori_loop(0, 4, pair_out, 0)

    def end_home(half):
        target = (second_end, first_end)[half]
        return rcopy(
            end_sum.at[half], end_got.at[half], end_last.at[half], end_last.at[2 + half], target
        )


    def to_peer(i, off):
        return rcopy(x_out.at[i], x_in.at[i], xs_send.at[i], xs_recv.at[i], peer(off))

    def finish(i):
        who = group_of(i)
        pl.when(has_up)(lambda: to_down(who).wait_recv())
        pl.when(has_down)(lambda: to_up(who).wait_recv())
        return accum[who] + from_above[who].astype(F32) + from_below[who].astype(F32)

    def along_x(half):
        for j in range(3):
            x_out[half * 3 + j] = finish(half * 4 + j).astype(BF16)
            to_peer(half * 3 + j, offs[j]).start()
        red[half] = finish(half * 4 + 3)

    along_x(0)

    def gathered(half):
        total = red[half]
        for j in range(3):
            to_peer(half * 3 + j, offs[j]).wait_recv()
            total = total + x_in[half * 3 + j].astype(F32)
        return total

    z_out[...] = gathered(0).astype(BF16)
    across_z = rcopy(z_out, z_in, zs_send.at[0], zs_recv.at[0], other)
    across_z.start()
    @pl.when(end)
    def _():
        for half in (1, 0):
            who = ((zh + 1 - half) % 2) * 4 + xi
            total = ghost_out[end_side, who].astype(F32)
            for j in range(3):
                end_peer(half * 3 + j).wait_recv()
                total = total + end_x[half * 3 + j].astype(F32)
            end_sum[half] = total.astype(BF16)
            end_home(half).start()

    along_x(1)

    def read_z(n, pos):
        value = ys[pos] * factor
        return value[0:8], value[8:16]

    rotate_out(read_z, wige, back, 1)
    wide = across(back, 1)
    first = wide.astype(BF16)
    second = (wide - first.astype(F32)).astype(BF16)
    agg = dot(first, sca_tile[...]) + dot(second, sca_tile[...])
    upd_ref[...] = from_rows(agg)

    red[1] = gathered(1)

    @pl.when(end)
    def _():
        end_home(0).wait_recv()
        end_home(1).wait_recv()
        red[1] = red[1] + (end_got[0].astype(F32) + end_got[1].astype(F32))

    for i in range(6):
        to_peer(i, offs[i % 3]).wait_send()
    for i in range(8):
        pl.when(has_down)(lambda i=i: to_down(i).wait_send())
        pl.when(has_up)(lambda i=i: to_up(i).wait_send())

    @pl.when(end)
    def _():
        for i in range(6):
            end_peer(i).wait_send()
        end_home(0).wait_send()
        end_home(1).wait_send()
    for copy, cond in sends:
        if cond is None:
            copy.wait_send()
        else:
            pl.when(cond)(lambda copy=copy: copy.wait_send())

    @pl.when(end)
    def _():
        for n, who in enumerate((mirror, ch)):
            for j, off in enumerate((2, 1, 3)):
                end_copy(n * 3 + j, who, peer(off)).wait_send()
    across_z.wait_send()
    across_z.wait_recv()
    grad = red[1] + z_in[...].astype(F32)
    grad_ref[...] = from_rows(grad)


def on_device(
    node_irreps,
    out_grad,
    edge_source,
    edge_rotation,
    edge_count,
    ghost_slot,
    wigner,
    so2_m0,
    so2_m1,
    so2_m2,
    attn_vector,
):
    vmem = pl.BlockSpec(memory_space=pltpu.VMEM)
    hbm = pl.BlockSpec(memory_space=pltpu.HBM)
    block = (ROWS, 128)
    dma = pltpu.SemaphoreType.DMA
    upd, grad = pl.pallas_call(
        body,
        out_shape=(
            jax.ShapeDtypeStruct((16, 16, K), F32),
            jax.ShapeDtypeStruct((16, 16, K), F32),
        ),
        in_specs=[hbm] * 11,
        out_specs=(vmem, vmem),
        scratch_shapes=[
            pltpu.VMEM((16, 16, K), BF16),
            pltpu.VMEM((16, 16, K), BF16),
            pltpu.VMEM((8, 16), jnp.int32),
            pltpu.VMEM((8, 16), jnp.int32),
            pltpu.SMEM((16,), jnp.int32),
            pltpu.SMEM((16,), jnp.int32),
            pltpu.VMEM((455, 256), F32),
            pltpu.VMEM((7, 7, 16, 128), BF16),
            pltpu.VMEM((2, 6, 6, 16, 128), BF16),
            pltpu.VMEM((2, 5, 5, 16, 128), BF16),
            pltpu.SMEM((16,), F32),
            dma((11,)),
            pltpu.VMEM((3, 8) + block, BF16),
            pltpu.VMEM((256, 128), F32),
            pltpu.VMEM((455, EDGES), F32),
            pltpu.VMEM((384, 1024), BF16),
            pltpu.VMEM((1024, 384), BF16),
            pltpu.VMEM((128, 1024), BF16),
            pltpu.VMEM((1024, 128), BF16),
            pltpu.VMEM((2, 8 * PITCH, 128), F32),
            pltpu.VMEM((2, 8 * PITCH, 128), F32),
            pltpu.VMEM((29 * 128, EDGES), BF16),
            pltpu.VMEM((29 * 128, EDGES), BF16),
            pltpu.VMEM((29, 16, EDGES), F32),
            pltpu.VMEM((29, 16, EDGES), F32),
            pltpu.VMEM((896, 128), BF16),
            pltpu.VMEM((768, 256), BF16),
            pltpu.VMEM((640, 256), BF16),
            pltpu.VMEM((8,) + block, F32),
            pltpu.VMEM((2, 8) + block, BF16),
            pltpu.VMEM((8,) + block, BF16),
            pltpu.VMEM((8,) + block, BF16),
            pltpu.VMEM((6,) + block, BF16),
            pltpu.VMEM((6,) + block, BF16),
            pltpu.VMEM(block, BF16),
            pltpu.VMEM(block, BF16),
            pltpu.VMEM((2,) + block, F32),
            pltpu.VMEM((6,) + block, BF16),
            pltpu.VMEM((2,) + block, BF16),
            pltpu.VMEM((2,) + block, BF16),
            dma((27,)),
            dma((3, 8)),
            dma((2, 8)),
            dma((2, 8)),
            dma((6,)),
            dma((6,)),
            dma((1,)),
            dma((1,)),
            dma((6,)),
            dma((6,)),
            dma((4,)),
        ],
        compiler_params=pltpu.CompilerParams(
            collective_id=0, has_side_effects=True, vmem_limit_bytes=24 * 1024 * 1024
        ),
        name="layer",
    )(
        *(
            pltpu.with_memory_space_constraint(array, pltpu.HBM)
            for array in (
                jnp.transpose(node_irreps, (1, 2, 0)),
                jnp.transpose(out_grad, (1, 2, 0)),
                edge_source,
                edge_rotation,
                edge_count,
                ghost_slot,
                wigner,
                jnp.transpose(so2_m0, (0, 2, 1, 3)),
                jnp.transpose(so2_m1, (0, 1, 3, 2, 4)),
                jnp.transpose(so2_m2, (0, 1, 3, 2, 4)),
                attn_vector,
            )
        )
    )
    updated = node_irreps.astype(F32) + jnp.transpose(upd, (2, 0, 1))
    irreps_grad = out_grad.astype(F32) + jnp.transpose(grad, (2, 0, 1))
    return updated.astype(BF16), irreps_grad


def solution(mesh):
    placed = (
        P(None, "ch", "dom"),
        P(None, "ch", "dom"),
        P(None, "dom"),
        P(None, "dom"),
        P("dom"),
        P("dom"),
        P(None, "dom"),
        P(None, "ch", None, None),
        P(None, None, "ch", None, None),
        P(None, None, "ch", None, None),
        P("ch"),
    )
    return jax.shard_map(
        on_device,
        mesh=mesh,
        in_specs=placed,
        out_specs=(P(None, "ch", "dom"), P(None, "ch", "dom")),
        check_vma=False,
    )
```
